16 devices in a mesh: dp: 2 (over y, z), row: 8 (over x, core).
Axes of the slice: x: 4, y: 2, z: 1, core: 2. Of those that a mesh axis runs over, the one named last changes fastest.
The devices are a block of a 4x4x8 slice.
Arguments:
- adjacency: bfloat16 [32768, 16384], P(('dp', 'row')), parts along dimension 0
- features: bfloat16 [32768, 602], P(('dp', 'row')), parts along dimension 0
- w_first: bfloat16 [602, 256], replicated
- w_second: bfloat16 [256, 41], replicated
Outputs:
- output: float32 [32768, 41], P(('dp', 'row')), parts along dimension 0
There are 2 independent parts. The reference program is written for one: setup_inputs(seed, part) draws one part's arguments, and reference() takes and returns one part's arrays. A program takes and returns all parts, laid end to end along the dimension named above; an argument that names none is the same for every part.
All inputs are finite; a program needn't handle non-finite values.
Results may differ from the reference program's by a relative error of at most 0.00189754.
Values are sent between devices in bfloat16 or wider.
A program may use at most 768 MiB of HBM per device.

```python
import jax
import jax.numpy as jnp

NODES = 16384
FEAT = 602
HIDDEN = 256
CLASSES = 41


def setup_inputs(seed: int = 0, part: int = 0) -> dict:
    key = jax.random.key(seed)
    key_adj, key_feat, key_first, key_second = jax.random.split(key, 4)
    adjacency = jax.random.normal(jax.random.fold_in(key_adj, part), (NODES, NODES), jnp.float32) * NODES ** -0.5
    features = jax.random.normal(jax.random.fold_in(key_feat, part), (NODES, FEAT), jnp.float32)
    w_first = jax.random.normal(key_first, (FEAT, HIDDEN), jnp.float32) * FEAT ** -0.5
    w_second = jax.random.normal(key_second, (HIDDEN, CLASSES), jnp.float32) * (2.0 / HIDDEN) ** 0.5
    return {'adjacency': adjacency.astype(jnp.bfloat16), 'features': features.astype(jnp.bfloat16), 'w_first': w_first.astype(jnp.bfloat16), 'w_second': w_second.astype(jnp.bfloat16)}


def reference(adjacency, features, w_first, w_second):
    z_first = jnp.dot(features, w_first, preferred_element_type=jnp.float32).astype(jnp.bfloat16)
    hidden = jnp.maximum(jnp.dot(adjacency, z_first, preferred_element_type=jnp.float32), 0.0).astype(jnp.bfloat16)
    z_second = jnp.dot(hidden, w_second, preferred_element_type=jnp.float32).astype(jnp.bfloat16)
    return jnp.maximum(jnp.dot(adjacency, z_second, preferred_element_type=jnp.float32), 0.0)
```

```python
import functools

import jax
import jax.numpy as jnp
from jax import lax
from jax.experimental import pallas as pl
from jax.experimental.pallas import tpu as pltpu
from jax.sharding import PartitionSpec as P

MESH = pl.DeviceIdType.MESH
CORES = 2
TILE = 256
F32, BF16 = jnp.float32, jnp.bfloat16

OWN, SIB, LEFT, RIGHT, SLEFT, SRIGHT, FAR, SFAR = range(8)
BLOCKS = 8
H0_RING = 4


def kernel(n, a_hbm, h0_hbm, w0_hbm, w1_hbm, out_hbm, slab, acc, h0_buf, w0_buf, w1_buf, z1t, h2t,
           a_sem, h0_sem, w_sem, z_recv, z_send, y_recv, y_send, out_sem):
    chips = n // CORES
    me = lax.axis_index("row")
    chip, core = me // CORES, me % CORES
    rows = acc.shape[0]
    pieces = rows // TILE
    half = pieces // 2
    zbase = slab.shape[0] - BLOCKS

    def device(step, flip):
        return (chip + step + chips) % chips * CORES + (core + flip) % CORES

    sib, left, right = device(0, 1), device(-1, 0), device(1, 0)

    def part(i):
        if isinstance(i, int):
            return pl.ds(i * TILE, TILE)
        return pl.ds(pl.multiple_of(i * TILE, TILE), TILE)

    def a_copy(owner, i, slot, sem):
        start = pl.multiple_of(owner * rows + i * TILE, TILE)
        return pltpu.make_async_copy(a_hbm.at[:, pl.ds(start, TILE)], slab.at[slot], a_sem.at[sem])

    def own_slab(i):
        return a_copy(me, i, i, i)

    def sib_slab(i):
        return a_copy(sib, i, pieces + i, pieces + i)

    def mid_slab(i, c):
        slot = 2 * pieces + 4 * i + c
        return a_copy(device(2 * (c % 2) - 1, c // 2), i, slot, slot)

    def far_slab(k, c):
        slot = 4 * k + c
        return a_copy(device(2, c // 2), 2 * k + c % 2, slot, slot)

    def z_ref(q, i):
        return slab.at[zbase + q, part(i)]

    def z_copy(src, dst, i, to, group):
        return pltpu.make_async_remote_copy(
            src_ref=z_ref(src, i), dst_ref=z_ref(dst, i), send_sem=z_send.at[group], recv_sem=z_recv.at[dst, i],
            device_id={"row": to}, device_id_type=MESH)

    def z_wait(q, i):
        z_copy(q, q, i, sib, 0).wait_recv()

    def z_sent(group, share):
        ref = slab.at[zbase, pl.ds(0, share * TILE)]
        pltpu.make_async_remote_copy(
            src_ref=ref, dst_ref=ref, send_sem=z_send.at[group], recv_sem=z_recv.at[0, 0],
            device_id={"row": sib}, device_id_type=MESH).wait_send()

    def y_copy(src, dst, h, to, group):
        return pltpu.make_async_remote_copy(
            src_ref=z1t.at[src, h], dst_ref=z1t.at[dst, h], send_sem=y_send.at[group, h], recv_sem=y_recv.at[dst, h],
            device_id={"row": to}, device_id_type=MESH)

    def y_wait(q, h):
        y_copy(q, q, h, sib, 0).wait_recv()

    def h0_copy(i):
        return pltpu.make_async_copy(h0_hbm.at[:, part(i)], h0_buf.at[i % H0_RING], h0_sem.at[i % H0_RING])

    w0_copy = pltpu.make_async_copy(w0_hbm, w0_buf, w_sem.at[0])
    w1_copy = pltpu.make_async_copy(w1_hbm, w1_buf, w_sem.at[1])
    w0_copy.start()
    for i in range(H0_RING):
        h0_copy(i).start()
    w1_copy.start()

    barrier = pltpu.get_barrier_semaphore()
    for peer in (sib, left, right):
        pl.semaphore_signal(barrier, inc=1, device_id={"row": peer}, device_id_type=MESH)

    @pl.loop(0, pieces)
    def _(i):
        own_slab(i).start()

    acc[...] = jnp.zeros_like(acc)
    w0_copy.wait()
    pl.semaphore_wait(barrier, 3)

    def send_own(i):
        z_copy(OWN, SIB, i, sib, 0).start()
        z_copy(OWN, LEFT, i, right, 1).start()
        z_copy(OWN, RIGHT, i, left, 2).start()

    @pl.loop(0, pieces)
    def _(i):
        h0_copy(i).wait()
        z = lax.dot_general(h0_buf[i % H0_RING], w0_buf[...], (((0,), (0,)), ((), ())), preferred_element_type=F32)
        slab[zbase + OWN, part(i)] = z.astype(BF16)

        @pl.when(i + H0_RING < pieces)
        def _():
            h0_copy(i + H0_RING).start()

        @pl.when(i > 0)
        def _():
            send_own(i - 1)

    @pl.loop(0, pieces)
    def _(i):
        sib_slab(i).start()

    w1_copy.wait()
    send_own(pieces - 1)

    def multiply(slot0, q0, i0, slot1, q1, i1):
        @pl.loop(0, pieces // 4)
        def _(jj):
            for u in range(4):
                r = part(4 * jj + u)
                acc[r, :] += (
                    jnp.dot(slab[slot0, r, :], slab[zbase + q0, part(i0)], preferred_element_type=F32)
                    + jnp.dot(slab[slot1, r, :], slab[zbase + q1, part(i1)], preferred_element_type=F32))

    @pl.loop(0, pieces // 2)
    def _(k):
        for u in range(2):
            own_slab(2 * k + u).wait()
            mid_slab((2 * k + u) // 4, (2 * k + u) % 4).start()
        multiply(2 * k, OWN, 2 * k, 2 * k + 1, OWN, 2 * k + 1)

    @pl.loop(0, pieces // 2)
    def _(k):
        for u in range(2):
            sib_slab(2 * k + u).wait()
            z_wait(SIB, 2 * k + u)
            mid_slab((pieces + 2 * k + u) // 4, (2 * k + u) % 4).start()
        multiply(pieces + 2 * k, SIB, 2 * k, pieces + 2 * k + 1, SIB, 2 * k + 1)

    def mid(i, even, ahead):
        base = 2 * pieces + 4 * i
        z_wait(LEFT, i)
        z_copy(LEFT, SLEFT, i, sib, 3).start()
        if even:
            z_copy(LEFT, FAR, i, right, 5).start()
        z_wait(RIGHT, i)
        z_copy(RIGHT, SRIGHT, i, sib, 4).start()
        if not even:
            z_copy(RIGHT, FAR, i, left, 6).start()
        for c in range(4):
            mid_slab(i, c).wait()
            ahead(c)
        multiply(base, LEFT, i, base + 1, RIGHT, i)
        z_wait(SLEFT, i)
        z_wait(SRIGHT, i)
        multiply(base + 2, SLEFT, i, base + 3, SRIGHT, i)

    @pl.loop(0, pieces // 4)
    def _(k):
        for u in range(2):
            i = 2 * k + u
            mid(i, u == 0, lambda c: mid_slab(i + half, c).start())

    @pl.loop(pieces // 4, pieces // 2)
    def _(k):
        for u in range(2):
            i = 2 * k + u
            mid(i, u == 0, lambda c: far_slab(i - half, c).start())

    z_sent(0, pieces)
    z_sent(1, pieces)
    z_sent(2, pieces)
    home = [zbase + q for q in (OWN, SIB, SLEFT, SRIGHT, LEFT, RIGHT, FAR, SFAR)]

    def again(owner, i):
        return a_copy(owner, i, home[i], 2 * pieces + i)

    for i in range(4):
        again(me, i).start()

    @pl.loop(0, pieces // 2)
    def _(k):
        for u in range(2):
            z_wait(FAR, 2 * k + u)
            z_copy(FAR, SFAR, 2 * k + u, sib, 7).start()
        for c in range(4):
            far_slab(k, c).wait()
        multiply(4 * k, FAR, 2 * k, 4 * k + 1, FAR, 2 * k + 1)
        for u in range(2):
            z_wait(SFAR, 2 * k + u)
        multiply(4 * k + 2, SFAR, 2 * k, 4 * k + 3, SFAR, 2 * k + 1)

    z_sent(3, pieces)
    z_sent(4, pieces)
    z_sent(5, pieces // 2)
    z_sent(6, pieces // 2)
    z_sent(7, pieces)
    for i in range(4, pieces):
        again(me, i).start()

    @pl.loop(0, pieces // 2)
    def _(jj):
        for u in range(2):
            j = 2 * jj + u
            hidden = jnp.maximum(acc[part(j), :], 0.0).astype(BF16)
            y = lax.dot_general(w1_buf[...], hidden, (((1,), (1,)), ((), ())), preferred_element_type=F32)
            z1t[OWN, j // half, j % half] = y.astype(BF16)

    y_copy(OWN, LEFT, 0, right, 1).start()
    y_copy(OWN, RIGHT, 1, left, 2).start()
    y_copy(OWN, SIB, 0, sib, 0).start()
    y_copy(OWN, SIB, 1, sib, 0).start()
    y_copy(OWN, LEFT, 1, right, 1).start()
    y_copy(OWN, RIGHT, 0, left, 2).start()

    h2t[...] = jnp.zeros_like(h2t)

    def second(q, h, slots):
        @pl.loop(0, pieces // 2)
        def _(jj):
            for u in range(2):
                j = 2 * jj + u
                total = h2t[j]
                for i in range(half):
                    total += lax.dot_general(
                        z1t[q, h, i], slab[slots[i], part(j), :], (((1,), (1,)), ((), ())),
                        preferred_element_type=F32)
                h2t[j] = total

    def mid_slots(c, h):
        return [2 * pieces + 4 * (h * half + i) + c for i in range(half)]

    def far_slots(c, h):
        return [4 * ((h * half + i) // 2) + 2 * c + (h * half + i) % 2 for i in range(half)]

    for h in range(2):
        for i in range(half):
            again(me, h * half + i).wait()
        second(OWN, h, home[h * half:(h + 1) * half])
        for i in range(half):
            again(sib, h * half + i).start()

    y_wait(LEFT, 0)
    y_copy(LEFT, FAR, 0, right, 5).start()
    y_copy(LEFT, SLEFT, 0, sib, 3).start()
    y_wait(RIGHT, 1)
    y_copy(RIGHT, FAR, 1, left, 6).start()
    y_copy(RIGHT, SRIGHT, 1, sib, 4).start()
    for h in range(2):
        y_wait(SIB, h)
        for i in range(half):
            again(sib, h * half + i).wait()
        second(SIB, h, home[h * half:(h + 1) * half])
    y_wait(LEFT, 1)
    y_copy(LEFT, SLEFT, 1, sib, 3).start()
    y_wait(RIGHT, 0)
    y_copy(RIGHT, SRIGHT, 0, sib, 4).start()
    second(LEFT, 0, mid_slots(0, 0))
    second(RIGHT, 1, mid_slots(1, 1))
    second(LEFT, 1, mid_slots(0, 1))
    y_wait(FAR, 0)
    y_copy(FAR, SFAR, 0, sib, 7).start()
    y_wait(FAR, 1)
    y_copy(FAR, SFAR, 1, sib, 7).start()
    second(RIGHT, 0, mid_slots(1, 0))
    for h in (0, 1):
        y_wait(SLEFT, h)
        second(SLEFT, h, mid_slots(2, h))
    for h in (1, 0):
        y_wait(SRIGHT, h)
        second(SRIGHT, h, mid_slots(3, h))
    second(FAR, 0, far_slots(0, 0))
    second(FAR, 1, far_slots(0, 1))
    for h in range(2):
        y_wait(SFAR, h)
        second(SFAR, h, far_slots(1, h))

    h2t[...] = jnp.maximum(h2t[...], 0.0)
    out_copies = [pltpu.make_async_copy(h2t.at[j], out_hbm.at[:, part(j)], out_sem.at[j]) for j in range(pieces)]
    for copy in out_copies:
        copy.start()
    for group in (0, 1, 2, 3, 4, 7):
        for h in range(2):
            y_copy(OWN, OWN, h, sib, group).wait_send()
    y_copy(OWN, OWN, 0, sib, 5).wait_send()
    y_copy(OWN, OWN, 1, sib, 6).wait_send()
    for copy in out_copies:
        copy.wait()


def solution(mesh):
    n = mesh.shape["row"]
    row_spec = P(("dp", "row"), None)
    full_spec = P(None, None)

    def per_device(adjacency, features, w_first, w_second):
        rows, feat, hidden, classes = features.shape[0], features.shape[1], w_first.shape[1], w_second.shape[1]
        pieces = rows // TILE
        resident = adjacency.shape[1] // TILE - 2 * pieces
        flops = 2 * rows * adjacency.shape[1] * (hidden + classes)
        out = pl.pallas_call(
            functools.partial(kernel, n),
            name="gcn",
            out_shape=jax.ShapeDtypeStruct((classes, rows), F32),
            in_specs=[pl.BlockSpec(memory_space=pl.ANY)] * 4,
            out_specs=pl.BlockSpec(memory_space=pl.ANY),
            scratch_shapes=[
                pltpu.VMEM((resident + BLOCKS, rows, TILE), BF16),
                pltpu.VMEM((rows, hidden), F32),
                pltpu.VMEM((H0_RING, feat, TILE), BF16),
                pltpu.VMEM((feat, hidden), BF16),
                pltpu.VMEM((classes, hidden), BF16),
                pltpu.VMEM((BLOCKS, 2, pieces // 2, classes, TILE), BF16),
                pltpu.VMEM((pieces, classes, TILE), F32),
                pltpu.SemaphoreType.DMA((resident,)),
                pltpu.SemaphoreType.DMA((H0_RING,)),
                pltpu.SemaphoreType.DMA((2,)),
                pltpu.SemaphoreType.DMA((BLOCKS, pieces)),
                pltpu.SemaphoreType.DMA((BLOCKS,)),
                pltpu.SemaphoreType.DMA((BLOCKS, 2)),
                pltpu.SemaphoreType.DMA((BLOCKS, 2)),
                pltpu.SemaphoreType.DMA((pieces,)),
            ],
            compiler_params=pltpu.CompilerParams(
                collective_id=0, has_side_effects=True, vmem_limit_bytes=67_043_328),
            cost_estimate=pl.CostEstimate(
                flops=flops, bytes_accessed=2 * adjacency.size, transcendentals=0),
        )(adjacency, features.T, w_first, w_second.T)
        return out.T

    return jax.shard_map(
        per_device, mesh=mesh, in_specs=(row_spec, row_spec, full_spec, full_spec), out_specs=row_spec,
        check_vma=False)
```

```python
import functools

import jax
import jax.numpy as jnp
from jax import lax
from jax.experimental import pallas as pl
from jax.experimental.pallas import tpu as pltpu
from jax.sharding import PartitionSpec as P

MESH = pl.DeviceIdType.MESH
CORES = 2
TILE = 256
F32, BF16 = jnp.float32, jnp.bfloat16

OWN, SIB, SLEFT, SRIGHT, LEFT, RIGHT, FAR, SFAR = range(8)
BLOCKS = 8
H0_RING = 4


def kernel(n, a_hbm, h0_hbm, w0_hbm, w1_hbm, out_hbm, slab, acc, h0_buf, w0_buf, w1_buf, z1t, h2t,
           a_sem, h0_sem, w_sem, z_recv, z_send, y_recv, y_send, out_sem):
    chips = n // CORES
    me = lax.axis_index("row")
    chip, core = me // CORES, me % CORES
    rows = acc.shape[0]
    pieces = rows // TILE
    half = pieces // 2
    zbase = slab.shape[0] - BLOCKS
    classes = w1_buf.shape[0]

    def device(step, flip):
        return (chip + step + chips) % chips * CORES + (core + flip) % CORES

    sib, left, right = device(0, 1), device(-1, 0), device(1, 0)

    def part(i):
        if isinstance(i, int):
            return pl.ds(i * TILE, TILE)
        return pl.ds(pl.multiple_of(i * TILE, TILE), TILE)

    def a_copy(owner, i, slot, sem):
        start = pl.multiple_of(owner * rows + i * TILE, TILE)
        return pltpu.make_async_copy(a_hbm.at[:, pl.ds(start, TILE)], slab.at[slot], a_sem.at[sem])

    def own_slab(i):
        return a_copy(me, i, i, i)

    def sib_slab(i):
        return a_copy(sib, i, pieces + i, pieces + i)

    def mid_slab(i, c):
        slot = 2 * pieces + 4 * i + c
        return a_copy(device(2 * (c % 2) - 1, c // 2), i, slot, slot)

    def far_slab(k, c):
        slot = 4 * k + c
        return a_copy(device(2, c // 2), 2 * k + c % 2, slot, slot)

    def z_ref(q, i):
        return slab.at[zbase + q, part(i)]

    def z_copy(src, dst, i, to, group):
        return pltpu.make_async_remote_copy(
            src_ref=z_ref(src, i), dst_ref=z_ref(dst, i), send_sem=z_send.at[group], recv_sem=z_recv.at[dst, i],
            device_id={"row": to}, device_id_type=MESH)

    def z_wait(q, i):
        z_copy(q, q, i, sib, 0).wait_recv()

    def z_sent(group, share):
        ref = slab.at[zbase, pl.ds(0, share * TILE)]
        pltpu.make_async_remote_copy(
            src_ref=ref, dst_ref=ref, send_sem=z_send.at[group], recv_sem=z_recv.at[0, 0],
            device_id={"row": sib}, device_id_type=MESH).wait_send()

    def y_copy(src, dst, h, to, group):
        return pltpu.make_async_remote_copy(
            src_ref=z1t.at[src, h], dst_ref=z1t.at[dst, h], send_sem=y_send.at[group, h], recv_sem=y_recv.at[dst, h],
            device_id={"row": to}, device_id_type=MESH)

    def y_wait(q, h):
        y_copy(q, q, h, sib, 0).wait_recv()

    def h0_copy(i):
        return pltpu.make_async_copy(h0_hbm.at[:, part(i)], h0_buf.at[i % H0_RING], h0_sem.at[i % H0_RING])

    w0_copy = pltpu.make_async_copy(w0_hbm, w0_buf, w_sem.at[0])
    w1_copy = pltpu.make_async_copy(w1_hbm, w1_buf, w_sem.at[1])
    w0_copy.start()
    for i in range(H0_RING):
        h0_copy(i).start()
    w1_copy.start()

    barrier = pltpu.get_barrier_semaphore()
    for peer in (sib, left, right):
        pl.semaphore_signal(barrier, inc=1, device_id={"row": peer}, device_id_type=MESH)

    @pl.loop(0, pieces)
    def _(i):
        own_slab(i).start()

    acc[...] = jnp.zeros_like(acc)
    w0_copy.wait()
    pl.semaphore_wait(barrier, 3)

    def send_own(i):
        z_copy(OWN, SIB, i, sib, 0).start()
        z_copy(OWN, LEFT, i, right, 1).start()
        z_copy(OWN, RIGHT, i, left, 2).start()

    @pl.loop(0, pieces)
    def _(i):
        h0_copy(i).wait()
        z = lax.dot_general(h0_buf[i % H0_RING], w0_buf[...], (((0,), (0,)), ((), ())), preferred_element_type=F32)
        slab[zbase + OWN, part(i)] = z.astype(BF16)

        @pl.when(i + H0_RING < pieces)
        def _():
            h0_copy(i + H0_RING).start()

        @pl.when(i > 0)
        def _():
            send_own(i - 1)

    @pl.loop(0, pieces)
    def _(i):
        sib_slab(i).start()

    w1_copy.wait()
    send_own(pieces - 1)

    def multiply(slot0, q0, i0, slot1, q1, i1):
        for j in range(pieces):
            r = part(j)
            acc[r, :] += (
                jnp.dot(slab[slot0, r, :], slab[zbase + q0, part(i0)], preferred_element_type=F32)
                + jnp.dot(slab[slot1, r, :], slab[zbase + q1, part(i1)], preferred_element_type=F32))

    @pl.loop(0, pieces // 2)
    def _(k):
        for u in range(2):
            own_slab(2 * k + u).wait()
            mid_slab((2 * k + u) // 4, (2 * k + u) % 4).start()
        multiply(2 * k, OWN, 2 * k, 2 * k + 1, OWN, 2 * k + 1)

    @pl.loop(0, pieces // 2)
    def _(k):
        for u in range(2):
            sib_slab(2 * k + u).wait()
            z_wait(SIB, 2 * k + u)
            mid_slab((pieces + 2 * k + u) // 4, (2 * k + u) % 4).start()
        multiply(pieces + 2 * k, SIB, 2 * k, pieces + 2 * k + 1, SIB, 2 * k + 1)

    def mid(i, even, ahead):
        base = 2 * pieces + 4 * i
        z_wait(LEFT, i)
        z_copy(LEFT, SLEFT, i, sib, 3).start()
        if even:
            z_copy(LEFT, FAR, i, right, 5).start()
        z_wait(RIGHT, i)
        z_copy(RIGHT, SRIGHT, i, sib, 4).start()
        if not even:
            z_copy(RIGHT, FAR, i, left, 6).start()
        for c in range(4):
            mid_slab(i, c).wait()
            ahead(c)
        multiply(base, LEFT, i, base + 1, RIGHT, i)
        z_wait(SLEFT, i)
        z_wait(SRIGHT, i)
        multiply(base + 2, SLEFT, i, base + 3, SRIGHT, i)

    @pl.loop(0, pieces // 4)
    def _(k):
        for u in range(2):
            i = 2 * k + u
            mid(i, u == 0, lambda c: mid_slab(i + half, c).start())

    @pl.loop(pieces // 4, pieces // 2)
    def _(k):
        for u in range(2):
            i = 2 * k + u
            mid(i, u == 0, lambda c: far_slab(i - half, c).start())

    z_sent(0, pieces)
    z_sent(1, pieces)
    z_sent(2, pieces)
    def again(owner, i):
        return a_copy(owner, i, zbase + i, 2 * pieces + i)

    for i in range(4):
        again(me, i).start()

    @pl.loop(0, pieces // 2)
    def _(k):
        for u in range(2):
            z_wait(FAR, 2 * k + u)
            z_copy(FAR, SFAR, 2 * k + u, sib, 7).start()
        for c in range(4):
            far_slab(k, c).wait()
        multiply(4 * k, FAR, 2 * k, 4 * k + 1, FAR, 2 * k + 1)
        for u in range(2):
            z_wait(SFAR, 2 * k + u)
        multiply(4 * k + 2, SFAR, 2 * k, 4 * k + 3, SFAR, 2 * k + 1)

    z_sent(3, pieces)
    z_sent(4, pieces)
    z_sent(5, pieces // 2)
    z_sent(6, pieces // 2)
    z_sent(7, pieces)
    for i in range(4, pieces):
        again(me, i).start()

    @pl.loop(0, pieces // 2)
    def _(jj):
        for u in range(2):
            j = 2 * jj + u
            hidden = jnp.maximum(acc[part(j), :], 0.0).astype(BF16)
            y = lax.dot_general(w1_buf[...], hidden, (((1,), (1,)), ((), ())), preferred_element_type=F32)
            z1t[OWN, j // half, j % half] = y.astype(BF16)

    y_copy(OWN, LEFT, 0, right, 1).start()
    y_copy(OWN, RIGHT, 1, left, 2).start()
    y_copy(OWN, SIB, 0, sib, 0).start()
    y_copy(OWN, SIB, 1, sib, 0).start()
    y_copy(OWN, LEFT, 1, right, 1).start()
    y_copy(OWN, RIGHT, 0, left, 2).start()

    def second(work, first=False):
        for j in range(pieces):
            total = None
            for q, h, i, slot in work:
                term = lax.dot_general(
                    slab[slot, part(j), :], z1t[q, h, i], (((1,), (1,)), ((), ())), preferred_element_type=F32)
                total = term if total is None else total + term
            if first:
                acc[part(j), 0:classes] = total
            else:
                acc[part(j), 0:classes] += total

    def pieces_of(q, h, slot_of):
        return [(q, h, i, slot_of(h * half + i)) for i in range(half)]

    def home(i):
        return zbase + i

    def mid_slot(c):
        return lambda i: 2 * pieces + 4 * i + c

    def far_slot(c):
        return lambda i: 4 * (i // 2) + 2 * c + i % 2

    for h in range(2):
        for i in range(half):
            again(me, h * half + i).wait()
        second(pieces_of(OWN, h, home), first=h == 0)
        for i in range(half):
            again(sib, h * half + i).start()
    y_wait(LEFT, 0)
    y_copy(LEFT, FAR, 0, right, 5).start()
    y_copy(LEFT, SLEFT, 0, sib, 3).start()
    y_wait(RIGHT, 1)
    y_copy(RIGHT, FAR, 1, left, 6).start()
    y_copy(RIGHT, SRIGHT, 1, sib, 4).start()
    second(pieces_of(LEFT, 0, mid_slot(0)) + pieces_of(RIGHT, 1, mid_slot(1)))
    y_wait(LEFT, 1)
    y_copy(LEFT, SLEFT, 1, sib, 3).start()
    y_wait(RIGHT, 0)
    y_copy(RIGHT, SRIGHT, 0, sib, 4).start()
    for h in range(2):
        y_wait(SIB, h)
    for i in range(pieces):
        again(sib, i).wait()
    second(pieces_of(SIB, 0, home) + pieces_of(SIB, 1, home))
    second(pieces_of(LEFT, 1, mid_slot(0)) + pieces_of(RIGHT, 0, mid_slot(1)))
    for h in range(2):
        y_wait(FAR, h)
        y_copy(FAR, SFAR, h, sib, 7).start()
    for h in range(2):
        y_wait(SLEFT, h)
        y_wait(SRIGHT, 1 - h)
        second(pieces_of(SLEFT, h, mid_slot(2)) + pieces_of(SRIGHT, 1 - h, mid_slot(3)))
    second(pieces_of(FAR, 0, far_slot(0)) + pieces_of(FAR, 1, far_slot(0)))
    for h in range(2):
        y_wait(SFAR, h)
    second(pieces_of(SFAR, 0, far_slot(1)) + pieces_of(SFAR, 1, far_slot(1)))
    for j in range(pieces):
        h2t[j] = jnp.maximum(acc[part(j), 0:128].T[0:classes], 0.0)

    out_copies = [pltpu.make_async_copy(h2t.at[j], out_hbm.at[:, part(j)], out_sem.at[j]) for j in range(pieces)]
    for copy in out_copies:
        copy.start()
    for group in (0, 1, 2, 3, 4, 7):
        for h in range(2):
            y_copy(OWN, OWN, h, sib, group).wait_send()
    y_copy(OWN, OWN, 0, sib, 5).wait_send()
    y_copy(OWN, OWN, 1, sib, 6).wait_send()
    for copy in out_copies:
        copy.wait()


def solution(mesh):
    n = mesh.shape["row"]
    row_spec = P(("dp", "row"), None)
    full_spec = P(None, None)

    def per_device(adjacency, features, w_first, w_second):
        rows, feat, hidden, classes = features.shape[0], features.shape[1], w_first.shape[1], w_second.shape[1]
        pieces = rows // TILE
        resident = adjacency.shape[1] // TILE - 2 * pieces
        flops = 2 * rows * adjacency.shape[1] * (hidden + classes)
        out = pl.pallas_call(
            functools.partial(kernel, n),
            name="gcn",
            out_shape=jax.ShapeDtypeStruct((classes, rows), F32),
            in_specs=[pl.BlockSpec(memory_space=pl.ANY)] * 4,
            out_specs=pl.BlockSpec(memory_space=pl.ANY),
            scratch_shapes=[
                pltpu.VMEM((resident + BLOCKS, rows, TILE), BF16),
                pltpu.VMEM((rows, hidden), F32),
                pltpu.VMEM((H0_RING, feat, TILE), BF16),
                pltpu.VMEM((feat, hidden), BF16),
                pltpu.VMEM((classes, hidden), BF16),
                pltpu.VMEM((BLOCKS, 2, pieces // 2, classes, TILE), BF16),
                pltpu.VMEM((pieces, classes, TILE), F32),
                pltpu.SemaphoreType.DMA((resident,)),
                pltpu.SemaphoreType.DMA((H0_RING,)),
                pltpu.SemaphoreType.DMA((2,)),
                pltpu.SemaphoreType.DMA((BLOCKS, pieces)),
                pltpu.SemaphoreType.DMA((BLOCKS,)),
                pltpu.SemaphoreType.DMA((BLOCKS, 2)),
                pltpu.SemaphoreType.DMA((BLOCKS, 2)),
                pltpu.SemaphoreType.DMA((pieces,)),
            ],
            compiler_params=pltpu.CompilerParams(
                collective_id=0, has_side_effects=True, vmem_limit_bytes=67_043_328),
            cost_estimate=pl.CostEstimate(
                flops=flops, bytes_accessed=2 * adjacency.size, transcendentals=0),
        )(adjacency, features.T, w_first, w_second.T)
        return out.T

    return jax.shard_map(
        per_device, mesh=mesh, in_specs=(row_spec, row_spec, full_spec, full_spec), out_specs=row_spec,
        check_vma=False)
```

```python
import functools

import jax
import jax.numpy as jnp
from jax import lax
from jax.experimental import pallas as pl
from jax.experimental.pallas import tpu as pltpu
from jax.sharding import PartitionSpec as P

MESH = pl.DeviceIdType.MESH
CORES = 2
TILE = 256
F32, BF16 = jnp.float32, jnp.bfloat16

OWN, SIB, SLEFT, SRIGHT, LEFT, RIGHT, FAR, SFAR = range(8)
BLOCKS = 8
H0_RING = 4
LANES = 128


def kernel(n, a_hbm, h0_hbm, w0_hbm, w1_hbm, out_hbm, slab, acc, h0_buf, w0_buf, w1_buf, w1_pad, z1t, h2t, out_buf,
           a_sem, h0_sem, w_sem, z_recv, z_send, y_recv, y_send, out_sem):
    chips = n // CORES
    me = lax.axis_index("row")
    chip, core = me // CORES, me % CORES
    rows = acc.shape[0]
    pieces = rows // TILE
    half = pieces // 2
    zbase = slab.shape[0] - BLOCKS
    classes = w1_buf.shape[0]

    def device(step, flip):
        return (chip + step + chips) % chips * CORES + (core + flip) % CORES

    sib, left, right = device(0, 1), device(-1, 0), device(1, 0)

    def part(i):
        if isinstance(i, int):
            return pl.ds(i * TILE, TILE)
        return pl.ds(pl.multiple_of(i * TILE, TILE), TILE)

    def a_copy(owner, i, slot, sem):
        start = pl.multiple_of(owner * rows + i * TILE, TILE)
        return pltpu.make_async_copy(a_hbm.at[:, pl.ds(start, TILE)], slab.at[slot], a_sem.at[sem])

    def own_slab(i):
        return a_copy(me, i, i, i)

    def sib_slab(i):
        return a_copy(sib, i, pieces + i, pieces + i)

    def mid_slab(i, c):
        slot = 2 * pieces + 4 * i + c
        return a_copy(device(2 * (c % 2) - 1, c // 2), i, slot, slot)

    def far_slab(k, c):
        slot = 4 * k + c
        return a_copy(device(2, c // 2), 2 * k + c % 2, slot, slot)

    def z_ref(q, i):
        return slab.at[zbase + q, part(i)]

    def z_copy(src, dst, i, to, group):
        return pltpu.make_async_remote_copy(
            src_ref=z_ref(src, i), dst_ref=z_ref(dst, i), send_sem=z_send.at[group], recv_sem=z_recv.at[dst, i],
            device_id={"row": to}, device_id_type=MESH)

    def z_wait(q, i):
        z_copy(q, q, i, sib, 0).wait_recv()

    def z_sent(group, share):
        ref = slab.at[zbase, pl.ds(0, share * TILE)]
        pltpu.make_async_remote_copy(
            src_ref=ref, dst_ref=ref, send_sem=z_send.at[group], recv_sem=z_recv.at[0, 0],
            device_id={"row": sib}, device_id_type=MESH).wait_send()

    def y_copy(src, dst, h, to, group):
        return pltpu.make_async_remote_copy(
            src_ref=z1t.at[src, h], dst_ref=z1t.at[dst, h], send_sem=y_send.at[group, h], recv_sem=y_recv.at[dst, h],
            device_id={"row": to}, device_id_type=MESH)

    def y_wait(q, h):
        y_copy(q, q, h, sib, 0).wait_recv()

    def h0_copy(i):
        return pltpu.make_async_copy(h0_hbm.at[:, part(i)], h0_buf.at[i % H0_RING], h0_sem.at[i % H0_RING])

    w0_copy = pltpu.make_async_copy(w0_hbm, w0_buf, w_sem.at[0])
    w1_copy = pltpu.make_async_copy(w1_hbm, w1_buf, w_sem.at[1])
    w0_copy.start()
    for i in range(H0_RING):
        h0_copy(i).start()
    w1_copy.start()

    barrier = pltpu.get_barrier_semaphore()
    for peer in (sib, left, right):
        pl.semaphore_signal(barrier, inc=1, device_id={"row": peer}, device_id_type=MESH)

    @pl.loop(0, pieces)
    def _(i):
        own_slab(i).start()

    acc[...] = jnp.zeros_like(acc)
    w1_pad[...] = jnp.zeros_like(w1_pad)
    w0_copy.wait()
    pl.semaphore_wait(barrier, 3)

    def send_own(i):
        z_copy(OWN, SIB, i, sib, 0).start()
        z_copy(OWN, LEFT, i, right, 1).start()
        z_copy(OWN, RIGHT, i, left, 2).start()

    @pl.loop(0, pieces)
    def _(i):
        h0_copy(i).wait()
        z = lax.dot_general(h0_buf[i % H0_RING], w0_buf[...], (((0,), (0,)), ((), ())), preferred_element_type=F32)
        slab[zbase + OWN, part(i)] = z.astype(BF16)

        @pl.when(i + H0_RING < pieces)
        def _():
            h0_copy(i + H0_RING).start()

        @pl.when(i > 0)
        def _():
            send_own(i - 1)

    @pl.loop(0, pieces)
    def _(i):
        sib_slab(i).start()

    w1_copy.wait()
    w1_pad[0:classes] = w1_buf[...]
    send_own(pieces - 1)

    def multiply(slot0, q0, i0, slot1, q1, i1, keep=True):
        slots, z = (slot0, slot1), (z_ref(q0, i0), z_ref(q1, i1))
        for j in range(pieces + 1):
            for u in range(2):
                if j < pieces:
                    acc[part(j), :] += jnp.dot(slab[slots[u], part(j), :], z[u][...], preferred_element_type=F32)
                if j > 0 and keep:
                    slab[slots[u], part(j - 1), :] = slab[slots[u], part(j - 1), :].T

    @pl.loop(0, pieces // 2)
    def _(k):
        for u in range(2):
            own_slab(2 * k + u).wait()
            mid_slab((2 * k + u) // 4, (2 * k + u) % 4).start()
        multiply(2 * k, OWN, 2 * k, 2 * k + 1, OWN, 2 * k + 1, keep=False)

    @pl.loop(0, pieces // 2)
    def _(k):
        for u in range(2):
            sib_slab(2 * k + u).wait()
            z_wait(SIB, 2 * k + u)
            mid_slab((pieces + 2 * k + u) // 4, (2 * k + u) % 4).start()
        multiply(pieces + 2 * k, SIB, 2 * k, pieces + 2 * k + 1, SIB, 2 * k + 1, keep=False)

    def mid(i, even, ahead):
        base = 2 * pieces + 4 * i
        z_wait(LEFT, i)
        z_copy(LEFT, SLEFT, i, sib, 3).start()
        if even:
            z_copy(LEFT, FAR, i, right, 5).start()
        z_wait(RIGHT, i)
        z_copy(RIGHT, SRIGHT, i, sib, 4).start()
        if not even:
            z_copy(RIGHT, FAR, i, left, 6).start()
        for c in range(4):
            mid_slab(i, c).wait()
            ahead(c)
        multiply(base, LEFT, i, base + 1, RIGHT, i)
        z_wait(SLEFT, i)
        z_wait(SRIGHT, i)
        multiply(base + 2, SLEFT, i, base + 3, SRIGHT, i)

    @pl.loop(0, pieces // 4)
    def _(k):
        for u in range(2):
            i = 2 * k + u
            mid(i, u == 0, lambda c: mid_slab(i + half, c).start())

    @pl.loop(pieces // 4, pieces // 2)
    def _(k):
        for u in range(2):
            i = 2 * k + u
            mid(i, u == 0, lambda c: far_slab(i - half, c).start())

    z_sent(0, pieces)
    z_sent(1, pieces)
    z_sent(2, pieces)
    def again(owner, i):
        return a_copy(owner, i, zbase + i, 2 * pieces + i)

    for i in range(4):
        again(me, i).start()

    def far(k, keep):
        for u in range(2):
            z_wait(FAR, 2 * k + u)
            z_copy(FAR, SFAR, 2 * k + u, sib, 7).start()
        for c in range(4):
            far_slab(k, c).wait()
        multiply(4 * k, FAR, 2 * k, 4 * k + 1, FAR, 2 * k + 1, keep)
        for u in range(2):
            z_wait(SFAR, 2 * k + u)
        multiply(4 * k + 2, SFAR, 2 * k, 4 * k + 3, SFAR, 2 * k + 1, keep)

    @pl.loop(0, pieces // 2 - 1)
    def _(k):
        far(k, True)

    far(pieces // 2 - 1, False)

    z_sent(3, pieces)
    z_sent(4, pieces)
    z_sent(5, pieces // 2)
    z_sent(6, pieces // 2)
    z_sent(7, pieces)
    for i in range(4, pieces):
        again(me, i).start()

    for j in range(pieces):
        hidden = jnp.maximum(acc[part(j), :], 0.0).astype(BF16)
        y = lax.dot_general(w1_pad[...], hidden, (((1,), (1,)), ((), ())), preferred_element_type=F32)
        z1t[OWN, j // half, j % half] = y.astype(BF16)

    y_copy(OWN, LEFT, 0, right, 1).start()
    y_copy(OWN, RIGHT, 1, left, 2).start()
    y_copy(OWN, SIB, 0, sib, 0).start()
    y_copy(OWN, SIB, 1, sib, 0).start()
    y_copy(OWN, LEFT, 1, right, 1).start()
    y_copy(OWN, RIGHT, 0, left, 2).start()

    def second(work, first=False):
        for j in range(pieces):
            total = None
            for q, h, i, slot in work:
                y = jnp.concatenate([z1t[q, h, i], jnp.zeros((LANES - z1t.shape[3], TILE), BF16)], axis=0)
                term = lax.dot_general(
                    slab[slot, part(j), :], y, (((1,), (1,)), ((), ())), preferred_element_type=F32)
                total = term if total is None else total + term
            if first:
                acc[part(j), 0:LANES] = total
            else:
                acc[part(j), 0:LANES] += total

    def second_turned(work, first=False):
        for j in range(pieces):
            total = None
            for q, h, i, slot in work:
                term = jnp.dot(z1t[q, h, i], slab[slot, part(j), :], preferred_element_type=F32)
                total = term if total is None else total + term
            if first:
                h2t[j] = total
            else:
                h2t[j] += total

    def pieces_of(q, h, slot_of):
        return [(q, h, i, slot_of(h * half + i)) for i in range(half)]

    def home(i):
        return zbase + i

    def mid_slot(c):
        return lambda i: 2 * pieces + 4 * i + c

    def far_slot(c):
        return lambda i: 4 * (i // 2) + 2 * c + i % 2

    for h in range(2):
        for i in range(half):
            again(me, h * half + i).wait()
        second(pieces_of(OWN, h, home), first=h == 0)
        for i in range(half):
            again(sib, h * half + i).start()
    y_wait(LEFT, 0)
    y_copy(LEFT, FAR, 0, right, 5).start()
    y_copy(LEFT, SLEFT, 0, sib, 3).start()
    y_wait(RIGHT, 1)
    y_copy(RIGHT, FAR, 1, left, 6).start()
    y_copy(RIGHT, SRIGHT, 1, sib, 4).start()
    second_turned(pieces_of(LEFT, 0, mid_slot(0)) + pieces_of(RIGHT, 1, mid_slot(1)), first=True)
    y_wait(LEFT, 1)
    y_copy(LEFT, SLEFT, 1, sib, 3).start()
    y_wait(RIGHT, 0)
    y_copy(RIGHT, SRIGHT, 0, sib, 4).start()
    for h in range(2):
        y_wait(SIB, h)
    for i in range(pieces):
        again(sib, i).wait()
    second(pieces_of(SIB, 0, home) + pieces_of(SIB, 1, home))
    second_turned(pieces_of(LEFT, 1, mid_slot(0)) + pieces_of(RIGHT, 0, mid_slot(1)))
    for h in range(2):
        y_wait(FAR, h)
        y_copy(FAR, SFAR, h, sib, 7).start()
    for h in range(2):
        y_wait(SLEFT, h)
        y_wait(SRIGHT, 1 - h)
        second_turned(pieces_of(SLEFT, h, mid_slot(2)) + pieces_of(SRIGHT, 1 - h, mid_slot(3)))
    far_work = pieces_of(FAR, 0, far_slot(0)) + pieces_of(FAR, 1, far_slot(0))
    sfar_work = pieces_of(SFAR, 0, far_slot(1)) + pieces_of(SFAR, 1, far_slot(1))
    second_turned(far_work[:-2])
    for h in range(2):
        y_wait(SFAR, h)
    second_turned(sfar_work[:-2])
    second(far_work[-2:] + sfar_work[-2:])
    for j in range(pieces):
        out_buf[j] = jnp.maximum(h2t[j, 0:classes] + acc[part(j), 0:LANES].T[0:classes], 0.0)

    out_copies = [pltpu.make_async_copy(out_buf.at[j], out_hbm.at[:, part(j)], out_sem.at[j]) for j in range(pieces)]
    for copy in out_copies:
        copy.start()
    for group in (0, 1, 2, 3, 4, 7):
        for h in range(2):
            y_copy(OWN, OWN, h, sib, group).wait_send()
    y_copy(OWN, OWN, 0, sib, 5).wait_send()
    y_copy(OWN, OWN, 1, sib, 6).wait_send()
    for copy in out_copies:
        copy.wait()


def solution(mesh):
    n = mesh.shape["row"]
    row_spec = P(("dp", "row"), None)
    full_spec = P(None, None)

    def per_device(adjacency, features, w_first, w_second):
        rows, feat, hidden, classes = features.shape[0], features.shape[1], w_first.shape[1], w_second.shape[1]
        pieces = rows // TILE
        padded = -(-classes // 16) * 16
        resident = adjacency.shape[1] // TILE - 2 * pieces
        flops = 2 * rows * adjacency.shape[1] * (hidden + classes)
        out = pl.pallas_call(
            functools.partial(kernel, n),
            name="gcn",
            out_shape=jax.ShapeDtypeStruct((classes, rows), F32),
            in_specs=[pl.BlockSpec(memory_space=pl.ANY)] * 4,
            out_specs=pl.BlockSpec(memory_space=pl.ANY),
            scratch_shapes=[
                pltpu.VMEM((resident + BLOCKS, rows, TILE), BF16),
                pltpu.VMEM((rows, hidden), F32),
                pltpu.VMEM((H0_RING, feat, TILE), BF16),
                pltpu.VMEM((feat, hidden), BF16),
                pltpu.VMEM((classes, hidden), BF16),
                pltpu.VMEM((padded, hidden), BF16),
                pltpu.VMEM((BLOCKS, 2, pieces // 2, padded, TILE), BF16),
                pltpu.VMEM((pieces, padded, TILE), F32),
                pltpu.VMEM((pieces, classes, TILE), F32),
                pltpu.SemaphoreType.DMA((resident,)),
                pltpu.SemaphoreType.DMA((H0_RING,)),
                pltpu.SemaphoreType.DMA((2,)),
                pltpu.SemaphoreType.DMA((BLOCKS, pieces)),
                pltpu.SemaphoreType.DMA((BLOCKS,)),
                pltpu.SemaphoreType.DMA((BLOCKS, 2)),
                pltpu.SemaphoreType.DMA((BLOCKS, 2)),
                pltpu.SemaphoreType.DMA((pieces,)),
            ],
            compiler_params=pltpu.CompilerParams(
                collective_id=0, has_side_effects=True, vmem_limit_bytes=67_043_328),
            cost_estimate=pl.CostEstimate(
                flops=flops, bytes_accessed=2 * adjacency.size, transcendentals=0),
        )(adjacency, features.T, w_first, w_second.T)
        return out.T

    return jax.shard_map(
        per_device, mesh=mesh, in_specs=(row_spec, row_spec, full_spec, full_spec), out_specs=row_spec,
        check_vma=False)
```

```python
import functools

import jax
import jax.numpy as jnp
from jax import lax
from jax.experimental import pallas as pl
from jax.experimental.pallas import tpu as pltpu
from jax.sharding import PartitionSpec as P

MESH = pl.DeviceIdType.MESH
CORES = 2
TILE = 256
F32, BF16 = jnp.float32, jnp.bfloat16

OWN, SIB, SLEFT, SRIGHT, LEFT, RIGHT, FAR, SFAR = range(8)
BLOCKS = 8
H0_RING = 4
LANES = 128


def kernel(n, a_hbm, h0_hbm, w0_hbm, w1_hbm, out_hbm, slab, acc, h0_buf, w0_buf, w1_buf, w1_pad, z1t, h2t, out_buf,
           a_sem, h0_sem, w_sem, z_recv, z_send, y_recv, y_send, out_sem):
    chips = n // CORES
    me = lax.axis_index("row")
    chip, core = me // CORES, me % CORES
    rows = acc.shape[0]
    pieces = rows // TILE
    half = pieces // 2
    zbase = slab.shape[0] - BLOCKS
    classes = w1_buf.shape[0]

    def device(step, flip):
        return (chip + step + chips) % chips * CORES + (core + flip) % CORES

    sib, left, right = device(0, 1), device(-1, 0), device(1, 0)

    def part(i):
        if isinstance(i, int):
            return pl.ds(i * TILE, TILE)
        return pl.ds(pl.multiple_of(i * TILE, TILE), TILE)

    def a_copy(owner, i, slot, sem):
        start = pl.multiple_of(owner * rows + i * TILE, TILE)
        return pltpu.make_async_copy(a_hbm.at[:, pl.ds(start, TILE)], slab.at[slot], a_sem.at[sem])

    def own_slab(i):
        return a_copy(me, i, i, i)

    def sib_slab(i):
        return a_copy(sib, i, pieces + i, pieces + i)

    def mid_slab(i, c):
        slot = 2 * pieces + 4 * i + c
        return a_copy(device(2 * (c % 2) - 1, c // 2), i, slot, slot)

    def far_slab(k, c):
        slot = 4 * k + c
        return a_copy(device(2, c // 2), 2 * k + c % 2, slot, slot)

    def z_ref(q, i):
        return slab.at[zbase + q, part(i)]

    def z_copy(src, dst, i, to, group):
        return pltpu.make_async_remote_copy(
            src_ref=z_ref(src, i), dst_ref=z_ref(dst, i), send_sem=z_send.at[group], recv_sem=z_recv.at[dst, i],
            device_id={"row": to}, device_id_type=MESH)

    def z_wait(q, i):
        z_copy(q, q, i, sib, 0).wait_recv()

    def z_sent(group, share):
        ref = slab.at[zbase, pl.ds(0, share * TILE)]
        pltpu.make_async_remote_copy(
            src_ref=ref, dst_ref=ref, send_sem=z_send.at[group], recv_sem=z_recv.at[0, 0],
            device_id={"row": sib}, device_id_type=MESH).wait_send()

    def y_copy(src, dst, h, to, group):
        return pltpu.make_async_remote_copy(
            src_ref=z1t.at[src, h], dst_ref=z1t.at[dst, h], send_sem=y_send.at[group, h], recv_sem=y_recv.at[dst, h],
            device_id={"row": to}, device_id_type=MESH)

    def y_wait(q, h):
        y_copy(q, q, h, sib, 0).wait_recv()

    def h0_copy(i):
        return pltpu.make_async_copy(h0_hbm.at[:, part(i)], h0_buf.at[i % H0_RING], h0_sem.at[i % H0_RING])

    w0_copy = pltpu.make_async_copy(w0_hbm, w0_buf, w_sem.at[0])
    w1_copy = pltpu.make_async_copy(w1_hbm, w1_buf, w_sem.at[1])
    w0_copy.start()
    for i in range(H0_RING):
        h0_copy(i).start()
    w1_copy.start()

    barrier = pltpu.get_barrier_semaphore()
    for peer in (sib, left, right):
        pl.semaphore_signal(barrier, inc=1, device_id={"row": peer}, device_id_type=MESH)

    @pl.loop(0, pieces)
    def _(i):
        own_slab(i).start()

    acc[...] = jnp.zeros_like(acc)
    w1_pad[...] = jnp.zeros_like(w1_pad)
    w0_copy.wait()

    def send_own(i):
        z_copy(OWN, SIB, i, sib, 0).start()
        z_copy(OWN, LEFT, i, right, 1).start()
        z_copy(OWN, RIGHT, i, left, 2).start()

    def feature(i):
        h0_copy(i).wait()
        z = lax.dot_general(h0_buf[i % H0_RING], w0_buf[...], (((0,), (0,)), ((), ())), preferred_element_type=F32)
        slab[zbase + OWN, part(i)] = z.astype(BF16)

        @pl.when(i + H0_RING < pieces)
        def _():
            h0_copy(i + H0_RING).start()

    feature(0)
    pl.semaphore_wait(barrier, 3)

    @pl.loop(1, pieces)
    def _(i):
        feature(i)
        send_own(i - 1)

    @pl.loop(0, pieces)
    def _(i):
        sib_slab(i).start()

    w1_copy.wait()
    w1_pad[0:classes] = w1_buf[...]
    send_own(pieces - 1)

    def multiply(slot0, q0, i0, slot1, q1, i1, keep=True):
        slots, z = (slot0, slot1), (z_ref(q0, i0), z_ref(q1, i1))
        for j in range(pieces + 1):
            for u in range(2):
                if j < pieces:
                    acc[part(j), :] += jnp.dot(slab[slots[u], part(j), :], z[u][...], preferred_element_type=F32)
                if j > 0 and keep:
                    slab[slots[u], part(j - 1), :] = slab[slots[u], part(j - 1), :].T

    @pl.loop(0, pieces // 2)
    def _(k):
        for u in range(2):
            own_slab(2 * k + u).wait()
            mid_slab((2 * k + u) // 4, (2 * k + u) % 4).start()
        multiply(2 * k, OWN, 2 * k, 2 * k + 1, OWN, 2 * k + 1, keep=False)

    @pl.loop(0, pieces // 2)
    def _(k):
        for u in range(2):
            sib_slab(2 * k + u).wait()
            z_wait(SIB, 2 * k + u)
            mid_slab((pieces + 2 * k + u) // 4, (2 * k + u) % 4).start()
        multiply(pieces + 2 * k, SIB, 2 * k, pieces + 2 * k + 1, SIB, 2 * k + 1, keep=False)

    def front(i, even):
        z_wait(LEFT, i)
        z_copy(LEFT, SLEFT, i, sib, 3).start()
        if even:
            z_copy(LEFT, FAR, i, right, 5).start()
        z_wait(RIGHT, i)
        z_copy(RIGHT, SRIGHT, i, sib, 4).start()
        if not even:
            z_copy(RIGHT, FAR, i, left, 6).start()
        for c in range(2):
            mid_slab(i, c).wait()

        @pl.when(i < half)
        def _():
            for c in range(4):
                mid_slab(i + half, c).start()

        @pl.when(i >= half)
        def _():
            for c in range(4):
                far_slab(i - half, c).start()

        base = 2 * pieces + 4 * i
        multiply(base, LEFT, i, base + 1, RIGHT, i)

    def back(i):
        for c in range(2, 4):
            mid_slab(i, c).wait()
        z_wait(SLEFT, i)
        z_wait(SRIGHT, i)
        base = 2 * pieces + 4 * i
        multiply(base + 2, SLEFT, i, base + 3, SRIGHT, i)

    @pl.loop(0, pieces // 2)
    def _(k):
        front(2 * k, True)

        @pl.when(k > 0)
        def _():
            back(2 * k - 1)

        front(2 * k + 1, False)
        back(2 * k)

    def far_front(k, keep=True):
        for u in range(2):
            z_wait(FAR, 2 * k + u)
            z_copy(FAR, SFAR, 2 * k + u, sib, 7).start()
        for c in range(2):
            far_slab(k, c).wait()
        multiply(4 * k, FAR, 2 * k, 4 * k + 1, FAR, 2 * k + 1, keep)

    def far_back(k, keep=True):
        for c in range(2, 4):
            far_slab(k, c).wait()
        for u in range(2):
            z_wait(SFAR, 2 * k + u)
        multiply(4 * k + 2, SFAR, 2 * k, 4 * k + 3, SFAR, 2 * k + 1, keep)

    far_front(0)
    back(pieces - 1)

    z_sent(0, pieces)
    z_sent(1, pieces)
    z_sent(2, pieces)

    def again(owner, i):
        return a_copy(owner, i, zbase + i, 2 * pieces + i)

    for i in range(4):
        again(me, i).start()

    @pl.loop(1, half - 1)
    def _(k):
        far_front(k)
        far_back(k - 1)

    far_front(half - 1, keep=False)
    far_back(half - 2)
    far_back(half - 1, keep=False)

    z_sent(3, pieces)
    z_sent(4, pieces)
    z_sent(5, pieces // 2)
    z_sent(6, pieces // 2)
    z_sent(7, pieces)
    for i in range(4, pieces):
        again(me, i).start()

    for j in range(pieces):
        hidden = jnp.maximum(acc[part(j), :], 0.0).astype(BF16)
        y = lax.dot_general(w1_pad[...], hidden, (((1,), (1,)), ((), ())), preferred_element_type=F32)
        z1t[OWN, j // half, j % half] = y.astype(BF16)

    y_copy(OWN, LEFT, 0, right, 1).start()
    y_copy(OWN, RIGHT, 1, left, 2).start()
    y_copy(OWN, SIB, 0, sib, 0).start()
    y_copy(OWN, SIB, 1, sib, 0).start()
    y_copy(OWN, LEFT, 1, right, 1).start()
    y_copy(OWN, RIGHT, 0, left, 2).start()

    def second(work, first=False):
        for j in range(pieces):
            total = None
            for q, h, i, slot in work:
                y = jnp.concatenate([z1t[q, h, i], jnp.zeros((LANES - z1t.shape[3], TILE), BF16)], axis=0)
                term = lax.dot_general(
                    slab[slot, part(j), :], y, (((1,), (1,)), ((), ())), preferred_element_type=F32)
                total = term if total is None else total + term
            if first:
                acc[part(j), 0:LANES] = total
            else:
                acc[part(j), 0:LANES] += total

    def second_turned(work, first=False):
        for j in range(pieces):
            total = None
            for q, h, i, slot in work:
                term = jnp.dot(z1t[q, h, i], slab[slot, part(j), :], preferred_element_type=F32)
                total = term if total is None else total + term
            if first:
                h2t[j] = total
            else:
                h2t[j] += total

    def pieces_of(q, h, slot_of):
        return [(q, h, i, slot_of(h * half + i)) for i in range(half)]

    def home(i):
        return zbase + i

    def mid_slot(c):
        return lambda i: 2 * pieces + 4 * i + c

    def far_slot(c):
        return lambda i: 4 * (i // 2) + 2 * c + i % 2

    for h in range(2):
        for i in range(half):
            again(me, h * half + i).wait()
        second(pieces_of(OWN, h, home), first=h == 0)
        for i in range(half):
            again(sib, h * half + i).start()
    y_wait(LEFT, 0)
    y_copy(LEFT, FAR, 0, right, 5).start()
    y_copy(LEFT, SLEFT, 0, sib, 3).start()
    y_wait(RIGHT, 1)
    y_copy(RIGHT, FAR, 1, left, 6).start()
    y_copy(RIGHT, SRIGHT, 1, sib, 4).start()
    second_turned(pieces_of(LEFT, 0, mid_slot(0)) + pieces_of(RIGHT, 1, mid_slot(1)), first=True)
    y_wait(LEFT, 1)
    y_copy(LEFT, SLEFT, 1, sib, 3).start()
    y_wait(RIGHT, 0)
    y_copy(RIGHT, SRIGHT, 0, sib, 4).start()
    for h in range(2):
        y_wait(SIB, h)
    for i in range(pieces):
        again(sib, i).wait()
    second(pieces_of(SIB, 0, home) + pieces_of(SIB, 1, home))
    second_turned(pieces_of(LEFT, 1, mid_slot(0)) + pieces_of(RIGHT, 0, mid_slot(1)))
    for h in range(2):
        y_wait(FAR, h)
        y_copy(FAR, SFAR, h, sib, 7).start()
    for h in range(2):
        y_wait(SLEFT, h)
        y_wait(SRIGHT, 1 - h)
        second_turned(pieces_of(SLEFT, h, mid_slot(2)) + pieces_of(SRIGHT, 1 - h, mid_slot(3)))
    far_work = pieces_of(FAR, 0, far_slot(0)) + pieces_of(FAR, 1, far_slot(0))
    sfar_work = pieces_of(SFAR, 0, far_slot(1)) + pieces_of(SFAR, 1, far_slot(1))
    second_turned(far_work[:-2])
    for h in range(2):
        y_wait(SFAR, h)
    second_turned(sfar_work[:-2])
    second(far_work[-2:] + sfar_work[-2:])
    for j in range(pieces):
        out_buf[j] = jnp.maximum(h2t[j, 0:classes] + acc[part(j), 0:LANES].T[0:classes], 0.0)

    out_copies = [pltpu.make_async_copy(out_buf.at[j], out_hbm.at[:, part(j)], out_sem.at[j]) for j in range(pieces)]
    for copy in out_copies:
        copy.start()
    for group in (0, 1, 2, 3, 4, 7):
        for h in range(2):
            y_copy(OWN, OWN, h, sib, group).wait_send()
    y_copy(OWN, OWN, 0, sib, 5).wait_send()
    y_copy(OWN, OWN, 1, sib, 6).wait_send()
    for copy in out_copies:
        copy.wait()


def solution(mesh):
    n = mesh.shape["row"]
    row_spec = P(("dp", "row"), None)
    full_spec = P(None, None)

    def per_device(adjacency, features, w_first, w_second):
        rows, feat, hidden, classes = features.shape[0], features.shape[1], w_first.shape[1], w_second.shape[1]
        pieces = rows // TILE
        padded = -(-classes // 16) * 16
        resident = adjacency.shape[1] // TILE - 2 * pieces
        flops = 2 * rows * adjacency.shape[1] * (hidden + classes)
        out = pl.pallas_call(
            functools.partial(kernel, n),
            name="gcn",
            out_shape=jax.ShapeDtypeStruct((classes, rows), F32),
            in_specs=[pl.BlockSpec(memory_space=pl.ANY)] * 4,
            out_specs=pl.BlockSpec(memory_space=pl.ANY),
            scratch_shapes=[
                pltpu.VMEM((resident + BLOCKS, rows, TILE), BF16),
                pltpu.VMEM((rows, hidden), F32),
                pltpu.VMEM((H0_RING, feat, TILE), BF16),
                pltpu.VMEM((feat, hidden), BF16),
                pltpu.VMEM((classes, hidden), BF16),
                pltpu.VMEM((padded, hidden), BF16),
                pltpu.VMEM((BLOCKS, 2, pieces // 2, padded, TILE), BF16),
                pltpu.VMEM((pieces, padded, TILE), F32),
                pltpu.VMEM((pieces, classes, TILE), F32),
                pltpu.SemaphoreType.DMA((resident,)),
                pltpu.SemaphoreType.DMA((H0_RING,)),
                pltpu.SemaphoreType.DMA((2,)),
                pltpu.SemaphoreType.DMA((BLOCKS, pieces)),
                pltpu.SemaphoreType.DMA((BLOCKS,)),
                pltpu.SemaphoreType.DMA((BLOCKS, 2)),
                pltpu.SemaphoreType.DMA((BLOCKS, 2)),
                pltpu.SemaphoreType.DMA((pieces,)),
            ],
            compiler_params=pltpu.CompilerParams(
                collective_id=0, has_side_effects=True, vmem_limit_bytes=67_043_328),
            cost_estimate=pl.CostEstimate(
                flops=flops, bytes_accessed=2 * adjacency.size, transcendentals=0),
        )(adjacency, features.T, w_first, w_second.T)
        return out.T

    return jax.shard_map(
        per_device, mesh=mesh, in_specs=(row_spec, row_spec, full_spec, full_spec), out_specs=row_spec,
        check_vma=False)
```

```python
import functools

import jax
import jax.numpy as jnp
from jax import lax
from jax.experimental import pallas as pl
from jax.experimental.pallas import tpu as pltpu
from jax.sharding import PartitionSpec as P

MESH = pl.DeviceIdType.MESH
CORES = 2
TILE = 256
F32, BF16 = jnp.float32, jnp.bfloat16

OWN, SIB, SLEFT, SRIGHT, LEFT, RIGHT, FAR, SFAR = range(8)
BLOCKS = 8
H0_RING = 4
LANES = 128


def kernel(n, a_hbm, h0_hbm, w0_hbm, w1_hbm, out_hbm, slab, acc, h0_buf, w0_buf, w1_buf, w1_pad, z1t, h2t, out_buf,
           a_sem, h0_sem, w_sem, z_recv, z_send, y_recv, y_send, out_sem):
    chips = n // CORES
    me = lax.axis_index("row")
    chip, core = me // CORES, me % CORES
    rows = acc.shape[0]
    pieces = rows // TILE
    half = pieces // 2
    zbase = slab.shape[0] - BLOCKS
    classes = w1_buf.shape[0]

    def device(step, flip):
        return (chip + step + chips) % chips * CORES + (core + flip) % CORES

    sib, left, right = device(0, 1), device(-1, 0), device(1, 0)

    def part(i):
        if isinstance(i, int):
            return pl.ds(i * TILE, TILE)
        return pl.ds(pl.multiple_of(i * TILE, TILE), TILE)

    def a_copy(owner, i, slot, sem):
        start = pl.multiple_of(owner * rows + i * TILE, TILE)
        return pltpu.make_async_copy(a_hbm.at[:, pl.ds(start, TILE)], slab.at[slot], a_sem.at[sem])

    def own_slab(i):
        return a_copy(me, i, i, i)

    def sib_slab(i):
        return a_copy(sib, i, pieces + i, pieces + i)

    def mid_slab(i, c):
        slot = 2 * pieces + 4 * i + c
        return a_copy(device(2 * (c % 2) - 1, c // 2), i, slot, slot)

    def far_slab(k, c):
        slot = 4 * k + c
        return a_copy(device(2, c // 2), 2 * k + c % 2, slot, slot)

    def z_ref(q, i):
        return slab.at[zbase + q, part(i)]

    def z_copy(src, dst, i, to, group):
        return pltpu.make_async_remote_copy(
            src_ref=z_ref(src, i), dst_ref=z_ref(dst, i), send_sem=z_send.at[group], recv_sem=z_recv.at[dst, i],
            device_id={"row": to}, device_id_type=MESH)

    def z_wait(q, i):
        z_copy(q, q, i, sib, 0).wait_recv()

    def z_sent(group, share):
        ref = slab.at[zbase, pl.ds(0, share * TILE)]
        pltpu.make_async_remote_copy(
            src_ref=ref, dst_ref=ref, send_sem=z_send.at[group], recv_sem=z_recv.at[0, 0],
            device_id={"row": sib}, device_id_type=MESH).wait_send()

    def y_copy(src, dst, h, to, group):
        return pltpu.make_async_remote_copy(
            src_ref=z1t.at[src, h], dst_ref=z1t.at[dst, h], send_sem=y_send.at[group, h], recv_sem=y_recv.at[dst, h],
            device_id={"row": to}, device_id_type=MESH)

    def y_wait(q, h):
        y_copy(q, q, h, sib, 0).wait_recv()

    def h0_copy(i):
        return pltpu.make_async_copy(h0_hbm.at[:, part(i)], h0_buf.at[i % H0_RING], h0_sem.at[i % H0_RING])

    w0_copy = pltpu.make_async_copy(w0_hbm, w0_buf, w_sem.at[0])
    w1_copy = pltpu.make_async_copy(w1_hbm, w1_buf, w_sem.at[1])
    w0_copy.start()
    for i in range(H0_RING):
        h0_copy(i).start()
    w1_copy.start()

    barrier = pltpu.get_barrier_semaphore()
    for peer in (sib, left, right):
        pl.semaphore_signal(barrier, inc=1, device_id={"row": peer}, device_id_type=MESH)

    @pl.loop(0, pieces)
    def _(i):
        own_slab(i).start()

    acc[...] = jnp.zeros_like(acc)
    w1_pad[...] = jnp.zeros_like(w1_pad)
    w0_copy.wait()

    def send_own(i):
        z_copy(OWN, SIB, i, sib, 0).start()
        z_copy(OWN, LEFT, i, right, 1).start()
        z_copy(OWN, RIGHT, i, left, 2).start()

    def feature(i):
        h0_copy(i).wait()
        z = lax.dot_general(h0_buf[i % H0_RING], w0_buf[...], (((0,), (0,)), ((), ())), preferred_element_type=F32)
        slab[zbase + OWN, part(i)] = z.astype(BF16)

        @pl.when(i + H0_RING < pieces)
        def _():
            h0_copy(i + H0_RING).start()

    feature(0)
    pl.semaphore_wait(barrier, 3)

    @pl.loop(1, pieces)
    def _(i):
        feature(i)
        send_own(i - 1)

    @pl.loop(0, pieces)
    def _(i):
        sib_slab(i).start()

    w1_copy.wait()
    w1_pad[0:classes] = w1_buf[...]
    send_own(pieces - 1)

    def multiply(slot0, q0, i0, slot1, q1, i1, keep=True):
        slots, z = (slot0, slot1), (z_ref(q0, i0), z_ref(q1, i1))
        for j in range(pieces + 1):
            for u in range(2):
                if j < pieces:
                    acc[part(j), :] += jnp.dot(slab[slots[u], part(j), :], z[u][...], preferred_element_type=F32)
                if j > 0 and keep:
                    slab[slots[u], part(j - 1), :] = slab[slots[u], part(j - 1), :].T

    @pl.loop(0, pieces // 2)
    def _(k):
        for u in range(2):
            own_slab(2 * k + u).wait()
            mid_slab((2 * k + u) // 4, (2 * k + u) % 4).start()
        multiply(2 * k, OWN, 2 * k, 2 * k + 1, OWN, 2 * k + 1, keep=False)

    @pl.loop(0, pieces // 2)
    def _(k):
        for u in range(2):
            sib_slab(2 * k + u).wait()
            z_wait(SIB, 2 * k + u)
            mid_slab((pieces + 2 * k + u) // 4, (2 * k + u) % 4).start()
        multiply(pieces + 2 * k, SIB, 2 * k, pieces + 2 * k + 1, SIB, 2 * k + 1, keep=False)

    def front(i, even):
        z_wait(LEFT, i)
        z_copy(LEFT, SLEFT, i, sib, 3).start()
        if even:
            z_copy(LEFT, FAR, i, right, 5).start()
        z_wait(RIGHT, i)
        z_copy(RIGHT, SRIGHT, i, sib, 4).start()
        if not even:
            z_copy(RIGHT, FAR, i, left, 6).start()
        for c in range(2):
            mid_slab(i, c).wait()

        @pl.when(i < half)
        def _():
            for c in range(4):
                mid_slab(i + half, c).start()

        @pl.when(i >= half)
        def _():
            for c in range(4):
                far_slab(i - half, c).start()

        base = 2 * pieces + 4 * i
        multiply(base, LEFT, i, base + 1, RIGHT, i)

    def back(i):
        for c in range(2, 4):
            mid_slab(i, c).wait()
        z_wait(SLEFT, i)
        z_wait(SRIGHT, i)
        base = 2 * pieces + 4 * i
        multiply(base + 2, SLEFT, i, base + 3, SRIGHT, i)

    @pl.loop(0, pieces // 2)
    def _(k):
        front(2 * k, True)

        @pl.when(k > 0)
        def _():
            back(2 * k - 1)

        front(2 * k + 1, False)
        back(2 * k)

    def far_front(k, keep=True):
        for u in range(2):
            z_wait(FAR, 2 * k + u)
            z_copy(FAR, SFAR, 2 * k + u, sib, 7).start()
        for c in range(2):
            far_slab(k, c).wait()
        multiply(4 * k, FAR, 2 * k, 4 * k + 1, FAR, 2 * k + 1, keep)

    def far_back(k, keep=True):
        for c in range(2, 4):
            far_slab(k, c).wait()
        for u in range(2):
            z_wait(SFAR, 2 * k + u)
        multiply(4 * k + 2, SFAR, 2 * k, 4 * k + 3, SFAR, 2 * k + 1, keep)

    far_front(0)
    back(pieces - 1)

    z_sent(0, pieces)
    z_sent(1, pieces)
    z_sent(2, pieces)

    def again(owner, i):
        return a_copy(owner, i, zbase + i, 2 * pieces + i)

    for i in range(4):
        again(me, i).start()

    far_back(0)

    @pl.loop(1, half - 1)
    def _(k):
        far_front(k)
        far_back(k)

    far_front(half - 1, keep=False)
    far_back(half - 1, keep=False)

    z_sent(3, pieces)
    z_sent(4, pieces)
    z_sent(5, pieces // 2)
    z_sent(6, pieces // 2)
    z_sent(7, pieces)
    for i in range(4, pieces):
        again(me, i).start()

    for j in range(pieces):
        hidden = jnp.maximum(acc[part(j), :], 0.0).astype(BF16)
        y = lax.dot_general(w1_pad[...], hidden, (((1,), (1,)), ((), ())), preferred_element_type=F32)
        z1t[OWN, j // half, j % half] = y.astype(BF16)

    y_copy(OWN, LEFT, 0, right, 1).start()
    y_copy(OWN, RIGHT, 1, left, 2).start()
    y_copy(OWN, SIB, 0, sib, 0).start()
    y_copy(OWN, SIB, 1, sib, 0).start()
    y_copy(OWN, LEFT, 1, right, 1).start()
    y_copy(OWN, RIGHT, 0, left, 2).start()

    def second(streamed, turned, first_streamed=False, first_turned=False):
        steps = max(len(streamed), 1)
        per = -(-len(turned) // steps)
        for j in range(pieces):
            down = across = None
            for k in range(steps):
                for q, h, i, slot in turned[k * per:(k + 1) * per]:
                    term = jnp.dot(z1t[q, h, i], slab[slot, part(j), :], preferred_element_type=F32)
                    across = term if across is None else across + term
                for q, h, i, slot in streamed[k:k + 1]:
                    y = jnp.concatenate([z1t[q, h, i], jnp.zeros((LANES - z1t.shape[3], TILE), BF16)], axis=0)
                    term = lax.dot_general(
                        slab[slot, part(j), :], y, (((1,), (1,)), ((), ())), preferred_element_type=F32)
                    down = term if down is None else down + term
            if down is not None:
                acc[part(j), 0:LANES] = down if first_streamed else acc[part(j), 0:LANES] + down
            if across is not None:
                h2t[j] = across if first_turned else h2t[j] + across

    def pieces_of(q, h, slot_of):
        return [(q, h, i, slot_of(h * half + i)) for i in range(half)]

    def home(i):
        return zbase + i

    def mid_slot(c):
        return lambda i: 2 * pieces + 4 * i + c

    def far_slot(c):
        return lambda i: 4 * (i // 2) + 2 * c + i % 2

    for h in range(2):
        for i in range(half):
            again(me, h * half + i).wait()
        second(pieces_of(OWN, h, home), [], first_streamed=h == 0)
        for i in range(half):
            again(sib, h * half + i).start()
    y_wait(LEFT, 0)
    y_copy(LEFT, FAR, 0, right, 5).start()
    y_copy(LEFT, SLEFT, 0, sib, 3).start()
    y_wait(RIGHT, 1)
    y_copy(RIGHT, FAR, 1, left, 6).start()
    y_copy(RIGHT, SRIGHT, 1, sib, 4).start()
    y_wait(SIB, 0)
    for i in range(half):
        again(sib, i).wait()
    second(pieces_of(SIB, 0, home), pieces_of(LEFT, 0, mid_slot(0)) + pieces_of(RIGHT, 1, mid_slot(1)), first_turned=True)
    y_wait(LEFT, 1)
    y_copy(LEFT, SLEFT, 1, sib, 3).start()
    y_wait(RIGHT, 0)
    y_copy(RIGHT, SRIGHT, 0, sib, 4).start()
    y_wait(SIB, 1)
    for i in range(half, pieces):
        again(sib, i).wait()
    second(pieces_of(SIB, 1, home), pieces_of(LEFT, 1, mid_slot(0)) + pieces_of(RIGHT, 0, mid_slot(1)))
    for h in range(2):
        y_wait(FAR, h)
        y_copy(FAR, SFAR, h, sib, 7).start()
    for h in range(2):
        y_wait(SLEFT, h)
        y_wait(SRIGHT, 1 - h)
    far_work = pieces_of(FAR, 0, far_slot(0)) + pieces_of(FAR, 1, far_slot(0))
    sfar_work = pieces_of(SFAR, 0, far_slot(1)) + pieces_of(SFAR, 1, far_slot(1))
    second([], pieces_of(SLEFT, 0, mid_slot(2)) + pieces_of(SRIGHT, 1, mid_slot(3)))
    second(far_work[-2:], pieces_of(SLEFT, 1, mid_slot(2)) + pieces_of(SRIGHT, 0, mid_slot(3)) + far_work[:-2])
    for h in range(2):
        y_wait(SFAR, h)
    second(sfar_work[-2:], sfar_work[:-2])
    for j in range(pieces):
        out_buf[j] = jnp.maximum(h2t[j, 0:classes] + acc[part(j), 0:LANES].T[0:classes], 0.0)

    out_copies = [pltpu.make_async_copy(out_buf.at[j], out_hbm.at[:, part(j)], out_sem.at[j]) for j in range(pieces)]
    for copy in out_copies:
        copy.start()
    for group in (0, 1, 2, 3, 4, 7):
        for h in range(2):
            y_copy(OWN, OWN, h, sib, group).wait_send()
    y_copy(OWN, OWN, 0, sib, 5).wait_send()
    y_copy(OWN, OWN, 1, sib, 6).wait_send()
    for copy in out_copies:
        copy.wait()


def solution(mesh):
    n = mesh.shape["row"]
    row_spec = P(("dp", "row"), None)
    full_spec = P(None, None)

    def per_device(adjacency, features, w_first, w_second):
        rows, feat, hidden, classes = features.shape[0], features.shape[1], w_first.shape[1], w_second.shape[1]
        pieces = rows // TILE
        padded = -(-classes // 16) * 16
        resident = adjacency.shape[1] // TILE - 2 * pieces
        flops = 2 * rows * adjacency.shape[1] * (hidden + classes)
        out = pl.pallas_call(
            functools.partial(kernel, n),
            name="gcn",
            out_shape=jax.ShapeDtypeStruct((classes, rows), F32),
            in_specs=[pl.BlockSpec(memory_space=pl.ANY)] * 4,
            out_specs=pl.BlockSpec(memory_space=pl.ANY),
            scratch_shapes=[
                pltpu.VMEM((resident + BLOCKS, rows, TILE), BF16),
                pltpu.VMEM((rows, hidden), F32),
                pltpu.VMEM((H0_RING, feat, TILE), BF16),
                pltpu.VMEM((feat, hidden), BF16),
                pltpu.VMEM((classes, hidden), BF16),
                pltpu.VMEM((padded, hidden), BF16),
                pltpu.VMEM((BLOCKS, 2, pieces // 2, padded, TILE), BF16),
                pltpu.VMEM((pieces, padded, TILE), F32),
                pltpu.VMEM((pieces, classes, TILE), F32),
                pltpu.SemaphoreType.DMA((resident,)),
                pltpu.SemaphoreType.DMA((H0_RING,)),
                pltpu.SemaphoreType.DMA((2,)),
                pltpu.SemaphoreType.DMA((BLOCKS, pieces)),
                pltpu.SemaphoreType.DMA((BLOCKS,)),
                pltpu.SemaphoreType.DMA((BLOCKS, 2)),
                pltpu.SemaphoreType.DMA((BLOCKS, 2)),
                pltpu.SemaphoreType.DMA((pieces,)),
            ],
            compiler_params=pltpu.CompilerParams(
                collective_id=0, has_side_effects=True, vmem_limit_bytes=67_043_328),
            cost_estimate=pl.CostEstimate(
                flops=flops, bytes_accessed=2 * adjacency.size, transcendentals=0),
        )(adjacency, features.T, w_first, w_second.T)
        return out.T

    return jax.shard_map(
        per_device, mesh=mesh, in_specs=(row_spec, row_spec, full_spec, full_spec), out_specs=row_spec,
        check_vma=False)
```

```python
import functools

import jax
import jax.numpy as jnp
from jax import lax
from jax.experimental import pallas as pl
from jax.experimental.pallas import tpu as pltpu
from jax.sharding import PartitionSpec as P

MESH = pl.DeviceIdType.MESH
CORES = 2
TILE = 256
F32, BF16 = jnp.float32, jnp.bfloat16

OWN, SIB, SLEFT, SRIGHT, LEFT, RIGHT, FAR, SFAR = range(8)
BLOCKS = 8
H0_RING = 4
LANES = 128


def kernel(n, a_hbm, h0_hbm, w0_hbm, w1_hbm, out_hbm, slab, acc, h0_buf, w0_buf, w1_buf, w1_pad, z1t, h2t, out_buf,
           a_sem, h0_sem, w_sem, z_recv, z_send, y_recv, y_send, out_sem):
    chips = n // CORES
    me = lax.axis_index("row")
    chip, core = me // CORES, me % CORES
    rows = acc.shape[0]
    pieces = rows // TILE
    half = pieces // 2
    zbase = slab.shape[0] - BLOCKS
    classes = w1_buf.shape[0]

    def device(step, flip):
        return (chip + step + chips) % chips * CORES + (core + flip) % CORES

    sib, left, right = device(0, 1), device(-1, 0), device(1, 0)

    def part(i):
        if isinstance(i, int):
            return pl.ds(i * TILE, TILE)
        return pl.ds(pl.multiple_of(i * TILE, TILE), TILE)

    def a_copy(owner, i, slot, sem):
        start = pl.multiple_of(owner * rows + i * TILE, TILE)
        return pltpu.make_async_copy(a_hbm.at[:, pl.ds(start, TILE)], slab.at[slot], a_sem.at[sem])

    def own_slab(i):
        return a_copy(me, i, i, i)

    def sib_slab(i):
        return a_copy(sib, i, pieces + i, pieces + i)

    def mid_slab(i, c):
        slot = 2 * pieces + 4 * i + c
        return a_copy(device(2 * (c % 2) - 1, c // 2), i, slot, slot)

    def far_slab(k, c):
        slot = 4 * k + c
        return a_copy(device(2, c // 2), 2 * k + c % 2, slot, slot)

    def z_ref(q, i):
        return slab.at[zbase + q, part(i)]

    def z_copy(src, dst, i, to, group):
        return pltpu.make_async_remote_copy(
            src_ref=z_ref(src, i), dst_ref=z_ref(dst, i), send_sem=z_send.at[group], recv_sem=z_recv.at[dst, i],
            device_id={"row": to}, device_id_type=MESH)

    def z_wait(q, i):
        z_copy(q, q, i, sib, 0).wait_recv()

    def z_sent(group, share):
        ref = slab.at[zbase, pl.ds(0, share * TILE)]
        pltpu.make_async_remote_copy(
            src_ref=ref, dst_ref=ref, send_sem=z_send.at[group], recv_sem=z_recv.at[0, 0],
            device_id={"row": sib}, device_id_type=MESH).wait_send()

    def y_copy(src, dst, h, to, group):
        return pltpu.make_async_remote_copy(
            src_ref=z1t.at[src, h], dst_ref=z1t.at[dst, h], send_sem=y_send.at[group, h], recv_sem=y_recv.at[dst, h],
            device_id={"row": to}, device_id_type=MESH)

    def y_wait(q, h):
        y_copy(q, q, h, sib, 0).wait_recv()

    def h0_copy(i):
        return pltpu.make_async_copy(h0_hbm.at[:, part(i)], h0_buf.at[i % H0_RING], h0_sem.at[i % H0_RING])

    w0_copy = pltpu.make_async_copy(w0_hbm, w0_buf, w_sem.at[0])
    w1_copy = pltpu.make_async_copy(w1_hbm, w1_buf, w_sem.at[1])
    w0_copy.start()
    for i in range(H0_RING):
        h0_copy(i).start()
    w1_copy.start()

    barrier = pltpu.get_barrier_semaphore()
    for peer in (sib, left, right):
        pl.semaphore_signal(barrier, inc=1, device_id={"row": peer}, device_id_type=MESH)

    @pl.loop(0, pieces)
    def _(i):
        own_slab(i).start()

    w0_copy.wait()

    def send_own(i):
        z_copy(OWN, SIB, i, sib, 0).start()
        z_copy(OWN, LEFT, i, right, 1).start()
        z_copy(OWN, RIGHT, i, left, 2).start()

    def feature(i):
        h0_copy(i).wait()
        z = lax.dot_general(h0_buf[i % H0_RING], w0_buf[...], (((0,), (0,)), ((), ())), preferred_element_type=F32)
        slab[zbase + OWN, part(i)] = z.astype(BF16)

        @pl.when(i + H0_RING < pieces)
        def _():
            h0_copy(i + H0_RING).start()

    feature(0)
    acc[...] = jnp.zeros_like(acc)
    w1_pad[...] = jnp.zeros_like(w1_pad)
    pl.semaphore_wait(barrier, 3)
    send_own(0)

    @pl.loop(1, pieces)
    def _(i):
        feature(i)

        @pl.when(i > 1)
        def _():
            send_own(i - 1)

    @pl.loop(0, pieces)
    def _(i):
        sib_slab(i).start()

    w1_copy.wait()
    w1_pad[0:classes] = w1_buf[...]
    send_own(pieces - 1)

    def multiply(slot0, q0, i0, slot1, q1, i1, keep=True):
        slots, z = (slot0, slot1), (z_ref(q0, i0), z_ref(q1, i1))
        for j in range(pieces + 1):
            for u in range(2):
                if j < pieces:
                    acc[part(j), :] += jnp.dot(slab[slots[u], part(j), :], z[u][...], preferred_element_type=F32)
                if j > 0 and keep:
                    slab[slots[u], part(j - 1), :] = slab[slots[u], part(j - 1), :].T

    @pl.loop(0, pieces // 2)
    def _(k):
        for u in range(2):
            own_slab(2 * k + u).wait()
            mid_slab((2 * k + u) // 4, (2 * k + u) % 4).start()
        multiply(2 * k, OWN, 2 * k, 2 * k + 1, OWN, 2 * k + 1, keep=False)

    @pl.loop(0, pieces // 2)
    def _(k):
        for u in range(2):
            sib_slab(2 * k + u).wait()
            z_wait(SIB, 2 * k + u)
            mid_slab((pieces + 2 * k + u) // 4, (2 * k + u) % 4).start()
        multiply(pieces + 2 * k, SIB, 2 * k, pieces + 2 * k + 1, SIB, 2 * k + 1, keep=False)

    def front(i, even):
        z_wait(LEFT, i)
        z_copy(LEFT, SLEFT, i, sib, 3).start()
        if even:
            z_copy(LEFT, FAR, i, right, 5).start()
        z_wait(RIGHT, i)
        z_copy(RIGHT, SRIGHT, i, sib, 4).start()
        if not even:
            z_copy(RIGHT, FAR, i, left, 6).start()
        for c in range(2):
            mid_slab(i, c).wait()

        @pl.when(i < half)
        def _():
            for c in range(4):
                mid_slab(i + half, c).start()

        @pl.when(i >= half)
        def _():
            for c in range(4):
                far_slab(i - half, c).start()

        base = 2 * pieces + 4 * i
        multiply(base, LEFT, i, base + 1, RIGHT, i)

    def back(i):
        for c in range(2, 4):
            mid_slab(i, c).wait()
        z_wait(SLEFT, i)
        z_wait(SRIGHT, i)
        base = 2 * pieces + 4 * i
        multiply(base + 2, SLEFT, i, base + 3, SRIGHT, i)

    @pl.loop(0, pieces // 2)
    def _(k):
        front(2 * k, True)

        @pl.when(k > 0)
        def _():
            back(2 * k - 1)

        front(2 * k + 1, False)
        back(2 * k)

    def far_front(k, keep=True):
        for u in range(2):
            z_wait(FAR, 2 * k + u)
            z_copy(FAR, SFAR, 2 * k + u, sib, 7).start()
        for c in range(2):
            far_slab(k, c).wait()
        multiply(4 * k, FAR, 2 * k, 4 * k + 1, FAR, 2 * k + 1, keep)

    def far_back(k, keep=True):
        for c in range(2, 4):
            far_slab(k, c).wait()
        for u in range(2):
            z_wait(SFAR, 2 * k + u)
        multiply(4 * k + 2, SFAR, 2 * k, 4 * k + 3, SFAR, 2 * k + 1, keep)

    far_front(0)
    back(pieces - 1)

    z_sent(0, pieces)
    z_sent(1, pieces)
    z_sent(2, pieces)

    def again(owner, i):
        return a_copy(owner, i, zbase + i, 2 * pieces + i)

    for i in range(4):
        again(me, i).start()

    far_back(0)

    @pl.loop(1, half - 1)
    def _(k):
        far_front(k)
        far_back(k)

    far_front(half - 1, keep=False)
    far_back(half - 1, keep=False)

    z_sent(3, pieces)
    z_sent(4, pieces)
    z_sent(5, pieces // 2)
    z_sent(6, pieces // 2)
    z_sent(7, pieces)
    for i in range(4, pieces):
        again(me, i).start()

    for j in range(pieces):
        hidden = jnp.maximum(acc[part(j), :], 0.0).astype(BF16)
        y = lax.dot_general(w1_pad[...], hidden, (((1,), (1,)), ((), ())), preferred_element_type=F32)
        z1t[OWN, j // half, j % half] = y.astype(BF16)

    y_copy(OWN, LEFT, 0, right, 1).start()
    y_copy(OWN, RIGHT, 1, left, 2).start()
    y_copy(OWN, SIB, 0, sib, 0).start()
    y_copy(OWN, SIB, 1, sib, 0).start()
    y_copy(OWN, LEFT, 1, right, 1).start()
    y_copy(OWN, RIGHT, 0, left, 2).start()

    def second(streamed, turned, first_streamed=False, first_turned=False):
        steps = max(len(streamed), 1)
        per = -(-len(turned) // steps)
        for j in range(pieces):
            down = across = None
            for k in range(steps):
                for q, h, i, slot in turned[k * per:(k + 1) * per]:
                    term = jnp.dot(z1t[q, h, i], slab[slot, part(j), :], preferred_element_type=F32)
                    across = term if across is None else across + term
                for q, h, i, slot in streamed[k:k + 1]:
                    y = jnp.concatenate([z1t[q, h, i], jnp.zeros((LANES - z1t.shape[3], TILE), BF16)], axis=0)
                    term = lax.dot_general(
                        slab[slot, part(j), :], y, (((1,), (1,)), ((), ())), preferred_element_type=F32)
                    down = term if down is None else down + term
            if down is not None:
                acc[part(j), 0:LANES] = down if first_streamed else acc[part(j), 0:LANES] + down
            if across is not None:
                h2t[j] = across if first_turned else h2t[j] + across

    def pieces_of(q, h, slot_of):
        return [(q, h, i, slot_of(h * half + i)) for i in range(half)]

    def home(i):
        return zbase + i

    def mid_slot(c):
        return lambda i: 2 * pieces + 4 * i + c

    def far_slot(c):
        return lambda i: 4 * (i // 2) + 2 * c + i % 2

    for h in range(2):
        for i in range(half):
            again(me, h * half + i).wait()
        second(pieces_of(OWN, h, home), [], first_streamed=h == 0)
        for i in range(half):
            again(sib, h * half + i).start()
    y_wait(LEFT, 0)
    y_copy(LEFT, FAR, 0, right, 5).start()
    y_copy(LEFT, SLEFT, 0, sib, 3).start()
    y_wait(RIGHT, 1)
    y_copy(RIGHT, FAR, 1, left, 6).start()
    y_copy(RIGHT, SRIGHT, 1, sib, 4).start()
    y_wait(SIB, 0)
    for i in range(half):
        again(sib, i).wait()
    second(pieces_of(SIB, 0, home), pieces_of(LEFT, 0, mid_slot(0)) + pieces_of(RIGHT, 1, mid_slot(1)), first_turned=True)
    y_wait(LEFT, 1)
    y_copy(LEFT, SLEFT, 1, sib, 3).start()
    y_wait(RIGHT, 0)
    y_copy(RIGHT, SRIGHT, 0, sib, 4).start()
    y_wait(SIB, 1)
    for i in range(half, pieces):
        again(sib, i).wait()
    second(pieces_of(SIB, 1, home), pieces_of(LEFT, 1, mid_slot(0)) + pieces_of(RIGHT, 0, mid_slot(1)))
    for h in range(2):
        y_wait(FAR, h)
        y_copy(FAR, SFAR, h, sib, 7).start()
    for h in range(2):
        y_wait(SLEFT, h)
        y_wait(SRIGHT, 1 - h)
    far_work = pieces_of(FAR, 0, far_slot(0)) + pieces_of(FAR, 1, far_slot(0))
    sfar_work = pieces_of(SFAR, 0, far_slot(1)) + pieces_of(SFAR, 1, far_slot(1))
    second([], pieces_of(SLEFT, 0, mid_slot(2)) + pieces_of(SRIGHT, 1, mid_slot(3)))
    second(far_work[-2:], pieces_of(SLEFT, 1, mid_slot(2)) + pieces_of(SRIGHT, 0, mid_slot(3)) + far_work[:-2])
    for h in range(2):
        y_wait(SFAR, h)
    second(sfar_work[-2:], sfar_work[:-2])
    for j in range(pieces):
        out_buf[j] = jnp.maximum(h2t[j, 0:classes] + acc[part(j), 0:LANES].T[0:classes], 0.0)

    out_copies = [pltpu.make_async_copy(out_buf.at[j], out_hbm.at[:, part(j)], out_sem.at[j]) for j in range(pieces)]
    for copy in out_copies:
        copy.start()
    for group in (0, 1, 2, 3, 4, 7):
        for h in range(2):
            y_copy(OWN, OWN, h, sib, group).wait_send()
    y_copy(OWN, OWN, 0, sib, 5).wait_send()
    y_copy(OWN, OWN, 1, sib, 6).wait_send()
    for copy in out_copies:
        copy.wait()


def solution(mesh):
    n = mesh.shape["row"]
    row_spec = P(("dp", "row"), None)
    full_spec = P(None, None)

    def per_device(adjacency, features, w_first, w_second):
        rows, feat, hidden, classes = features.shape[0], features.shape[1], w_first.shape[1], w_second.shape[1]
        pieces = rows // TILE
        padded = -(-classes // 16) * 16
        resident = adjacency.shape[1] // TILE - 2 * pieces
        flops = 2 * rows * adjacency.shape[1] * (hidden + classes)
        out = pl.pallas_call(
            functools.partial(kernel, n),
            name="gcn",
            out_shape=jax.ShapeDtypeStruct((classes, rows), F32),
            in_specs=[pl.BlockSpec(memory_space=pl.ANY)] * 4,
            out_specs=pl.BlockSpec(memory_space=pl.ANY),
            scratch_shapes=[
                pltpu.VMEM((resident + BLOCKS, rows, TILE), BF16),
                pltpu.VMEM((rows, hidden), F32),
                pltpu.VMEM((H0_RING, feat, TILE), BF16),
                pltpu.VMEM((feat, hidden), BF16),
                pltpu.VMEM((classes, hidden), BF16),
                pltpu.VMEM((padded, hidden), BF16),
                pltpu.VMEM((BLOCKS, 2, pieces // 2, padded, TILE), BF16),
                pltpu.VMEM((pieces, padded, TILE), F32),
                pltpu.VMEM((pieces, classes, TILE), F32),
                pltpu.SemaphoreType.DMA((resident,)),
                pltpu.SemaphoreType.DMA((H0_RING,)),
                pltpu.SemaphoreType.DMA((2,)),
                pltpu.SemaphoreType.DMA((BLOCKS, pieces)),
                pltpu.SemaphoreType.DMA((BLOCKS,)),
                pltpu.SemaphoreType.DMA((BLOCKS, 2)),
                pltpu.SemaphoreType.DMA((BLOCKS, 2)),
                pltpu.SemaphoreType.DMA((pieces,)),
            ],
            compiler_params=pltpu.CompilerParams(
                collective_id=0, has_side_effects=True, vmem_limit_bytes=67_043_328),
            cost_estimate=pl.CostEstimate(
                flops=flops, bytes_accessed=2 * adjacency.size, transcendentals=0),
        )(adjacency, features.T, w_first, w_second.T)
        return out.T

    return jax.shard_map(
        per_device, mesh=mesh, in_specs=(row_spec, row_spec, full_spec, full_spec), out_specs=row_spec,
        check_vma=False)
```

```python
import functools

import jax
import jax.numpy as jnp
from jax import lax
from jax.experimental import pallas as pl
from jax.experimental.pallas import tpu as pltpu
from jax.sharding import PartitionSpec as P

MESH = pl.DeviceIdType.MESH
CORES = 2
TILE = 256
F32, BF16 = jnp.float32, jnp.bfloat16

OWN, SIB, SLEFT, SRIGHT, LEFT, RIGHT, FAR, SFAR = range(8)
BLOCKS = 8
H0_RING = 2
EXTRA = 2
LANES = 128


def kernel(n, a_hbm, h0_hbm, w0_hbm, w1_hbm, out_hbm, slab, acc, h0_buf, w0_buf, w1_buf, w1_pad, z1t, h2t, out_buf,
           a_sem, h0_sem, w_sem, z_recv, z_send, y_recv, y_send, out_sem):
    chips = n // CORES
    me = lax.axis_index("row")
    chip, core = me // CORES, me % CORES
    rows = acc.shape[0]
    pieces = rows // TILE
    half = pieces // 2
    zbase = slab.shape[0] - BLOCKS
    classes = w1_buf.shape[0]

    def device(step, flip):
        return (chip + step + chips) % chips * CORES + (core + flip) % CORES

    sib, left, right = device(0, 1), device(-1, 0), device(1, 0)

    def part(i):
        if isinstance(i, int):
            return pl.ds(i * TILE, TILE)
        return pl.ds(pl.multiple_of(i * TILE, TILE), TILE)

    def a_copy(owner, i, slot, sem):
        start = pl.multiple_of(owner * rows + i * TILE, TILE)
        return pltpu.make_async_copy(a_hbm.at[:, pl.ds(start, TILE)], slab.at[slot], a_sem.at[sem])

    def own_slab(i):
        return a_copy(me, i, i, i)

    def sib_slab(i):
        return a_copy(sib, i, pieces + i, pieces + i)

    def mid_slab(i, c):
        slot = 2 * pieces + 4 * i + c
        return a_copy(device(2 * (c % 2) - 1, c // 2), i, slot, slot)

    def far_place(k, c):
        last = 4 * (half - 1) + 2
        return 4 * k + c + (c // 2) * (k // (half - 1)) * (zbase - EXTRA - last)

    def far_slab(k, c):
        slot = far_place(k, c)
        return a_copy(device(2, c // 2), 2 * k + c % 2, slot, slot)

    def z_ref(q, i):
        return slab.at[zbase + q, part(i)]

    def z_copy(src, dst, i, to, group):
        return pltpu.make_async_remote_copy(
            src_ref=z_ref(src, i), dst_ref=z_ref(dst, i), send_sem=z_send.at[group], recv_sem=z_recv.at[dst, i],
            device_id={"row": to}, device_id_type=MESH)

    def z_wait(q, i):
        z_copy(q, q, i, sib, 0).wait_recv()

    def z_sent(group, share):
        ref = slab.at[zbase, pl.ds(0, share * TILE)]
        pltpu.make_async_remote_copy(
            src_ref=ref, dst_ref=ref, send_sem=z_send.at[group], recv_sem=z_recv.at[0, 0],
            device_id={"row": sib}, device_id_type=MESH).wait_send()

    def y_copy(src, dst, h, to, group):
        return pltpu.make_async_remote_copy(
            src_ref=z1t.at[src, h], dst_ref=z1t.at[dst, h], send_sem=y_send.at[group, h], recv_sem=y_recv.at[dst, h],
            device_id={"row": to}, device_id_type=MESH)

    def y_wait(q, h):
        y_copy(q, q, h, sib, 0).wait_recv()

    def h0_copy(i):
        return pltpu.make_async_copy(h0_hbm.at[:, part(i)], h0_buf.at[i % H0_RING], h0_sem.at[i % H0_RING])

    w0_copy = pltpu.make_async_copy(w0_hbm, w0_buf, w_sem.at[0])
    w1_copy = pltpu.make_async_copy(w1_hbm, w1_buf, w_sem.at[1])
    w0_copy.start()
    for i in range(H0_RING):
        h0_copy(i).start()
    w1_copy.start()

    barrier = pltpu.get_barrier_semaphore()
    for peer in (sib, left, right):
        pl.semaphore_signal(barrier, inc=1, device_id={"row": peer}, device_id_type=MESH)

    @pl.loop(0, pieces)
    def _(i):
        own_slab(i).start()

    w0_copy.wait()

    def send_own(i):
        z_copy(OWN, SIB, i, sib, 0).start()
        z_copy(OWN, LEFT, i, right, 1).start()
        z_copy(OWN, RIGHT, i, left, 2).start()

    def feature(i):
        h0_copy(i).wait()
        z = lax.dot_general(h0_buf[i % H0_RING], w0_buf[...], (((0,), (0,)), ((), ())), preferred_element_type=F32)
        slab[zbase + OWN, part(i)] = z.astype(BF16)

        @pl.when(i + H0_RING < pieces)
        def _():
            h0_copy(i + H0_RING).start()

    feature(0)
    acc[...] = jnp.zeros_like(acc)
    w1_pad[...] = jnp.zeros_like(w1_pad)
    pl.semaphore_wait(barrier, 3)
    send_own(0)

    @pl.loop(1, pieces)
    def _(i):
        feature(i)

        @pl.when(i > 1)
        def _():
            send_own(i - 1)

    @pl.loop(0, pieces)
    def _(i):
        sib_slab(i).start()

    w1_copy.wait()
    w1_pad[0:classes] = w1_buf[...]
    send_own(pieces - 1)

    def multiply(slot0, q0, i0, slot1, q1, i1, keep=True):
        slots, z = (slot0, slot1), (z_ref(q0, i0), z_ref(q1, i1))
        for j in range(pieces + 1):
            for u in range(2):
                if j < pieces:
                    acc[part(j), :] += jnp.dot(slab[slots[u], part(j), :], z[u][...], preferred_element_type=F32)
                if j > 0 and keep:
                    slab[slots[u], part(j - 1), :] = slab[slots[u], part(j - 1), :].T

    @pl.loop(0, pieces // 2)
    def _(k):
        for u in range(2):
            own_slab(2 * k + u).wait()
            mid_slab((2 * k + u) // 4, (2 * k + u) % 4).start()
        multiply(2 * k, OWN, 2 * k, 2 * k + 1, OWN, 2 * k + 1, keep=False)

    @pl.loop(0, pieces // 2)
    def _(k):
        for u in range(2):
            sib_slab(2 * k + u).wait()
            z_wait(SIB, 2 * k + u)
            mid_slab((pieces + 2 * k + u) // 4, (2 * k + u) % 4).start()
        multiply(pieces + 2 * k, SIB, 2 * k, pieces + 2 * k + 1, SIB, 2 * k + 1, keep=False)

    def front(i, even):
        z_wait(LEFT, i)
        z_copy(LEFT, SLEFT, i, sib, 3).start()
        if even:
            z_copy(LEFT, FAR, i, right, 5).start()
        z_wait(RIGHT, i)
        z_copy(RIGHT, SRIGHT, i, sib, 4).start()
        if not even:
            z_copy(RIGHT, FAR, i, left, 6).start()
        for c in range(2):
            mid_slab(i, c).wait()

        @pl.when(i < half)
        def _():
            for c in range(4):
                mid_slab(i + half, c).start()

        @pl.when(i >= half)
        def _():
            for c in range(4):
                far_slab(i - half, c).start()

        base = 2 * pieces + 4 * i
        multiply(base, LEFT, i, base + 1, RIGHT, i)

    def back(i):
        for c in range(2, 4):
            mid_slab(i, c).wait()
        z_wait(SLEFT, i)
        z_wait(SRIGHT, i)
        base = 2 * pieces + 4 * i
        multiply(base + 2, SLEFT, i, base + 3, SRIGHT, i)

    @pl.loop(0, pieces // 2)
    def _(k):
        front(2 * k, True)

        @pl.when(k > 0)
        def _():
            back(2 * k - 1)

        front(2 * k + 1, False)
        back(2 * k)

    def far_front(k, keep=True):
        for u in range(2):
            z_wait(FAR, 2 * k + u)
            z_copy(FAR, SFAR, 2 * k + u, sib, 7).start()
        for c in range(2):
            far_slab(k, c).wait()
        multiply(4 * k, FAR, 2 * k, 4 * k + 1, FAR, 2 * k + 1, keep)

    def far_back(k, keep=True):
        for c in range(2, 4):
            far_slab(k, c).wait()
        for u in range(2):
            z_wait(SFAR, 2 * k + u)
        multiply(far_place(k, 2), SFAR, 2 * k, far_place(k, 3), SFAR, 2 * k + 1, keep)

    far_front(0)
    back(pieces - 1)

    z_sent(0, pieces)
    z_sent(1, pieces)
    z_sent(2, pieces)

    def again(owner, i):
        return a_copy(owner, i, zbase + i, 2 * pieces + i)

    for i in range(4):
        again(me, i).start()

    far_back(0)

    @pl.loop(1, half - 1)
    def _(k):
        far_front(k)
        far_back(k)

    far_front(half - 1, keep=False)
    far_back(half - 1, keep=False)

    z_sent(3, pieces)
    z_sent(4, pieces)
    z_sent(5, pieces // 2)
    z_sent(6, pieces // 2)
    z_sent(7, pieces)
    for i in range(4, pieces):
        again(me, i).start()

    for j in range(pieces):
        hidden = jnp.maximum(acc[part(j), :], 0.0).astype(BF16)
        y = lax.dot_general(w1_pad[...], hidden, (((1,), (1,)), ((), ())), preferred_element_type=F32)
        z1t[OWN, j // half, j % half] = y.astype(BF16)

    y_copy(OWN, LEFT, 0, right, 1).start()
    y_copy(OWN, RIGHT, 1, left, 2).start()
    y_copy(OWN, SIB, 0, sib, 0).start()
    y_copy(OWN, SIB, 1, sib, 0).start()
    y_copy(OWN, LEFT, 1, right, 1).start()
    y_copy(OWN, RIGHT, 0, left, 2).start()

    def second(streamed, turned, first_streamed=False, first_turned=False):
        steps = max(len(streamed), 1)
        per = -(-len(turned) // steps)
        for j in range(pieces):
            down = across = None
            for k in range(steps):
                for q, h, i, slot in turned[k * per:(k + 1) * per]:
                    term = jnp.dot(z1t[q, h, i], slab[slot, part(j), :], preferred_element_type=F32)
                    across = term if across is None else across + term
                for q, h, i, slot in streamed[k:k + 1]:
                    y = jnp.concatenate([z1t[q, h, i], jnp.zeros((LANES - z1t.shape[3], TILE), BF16)], axis=0)
                    term = lax.dot_general(
                        slab[slot, part(j), :], y, (((1,), (1,)), ((), ())), preferred_element_type=F32)
                    down = term if down is None else down + term
            if down is not None:
                acc[part(j), 0:LANES] = down if first_streamed else acc[part(j), 0:LANES] + down
            if across is not None:
                h2t[j] = across if first_turned else h2t[j] + across

    def pieces_of(q, h, slot_of):
        return [(q, h, i, slot_of(h * half + i)) for i in range(half)]

    def home(i):
        return zbase + i

    def mid_slot(c):
        return lambda i: 2 * pieces + 4 * i + c

    def far_slot(c):
        return lambda i: far_place(i // 2, 2 * c + i % 2)

    for h in range(2):
        for i in range(half):
            again(me, h * half + i).wait()
        second(pieces_of(OWN, h, home), [], first_streamed=h == 0)
        for i in range(h * half, min((h + 1) * half, pieces - EXTRA)):
            again(sib, i).start()
    y_wait(SIB, 0)
    y_wait(SIB, 1)
    kept = [(SIB, 1, i % half, pieces + i) for i in range(pieces - EXTRA, pieces)]
    second(kept, [])
    y_wait(LEFT, 0)
    y_copy(LEFT, FAR, 0, right, 5).start()
    y_copy(LEFT, SLEFT, 0, sib, 3).start()
    y_wait(RIGHT, 1)
    y_copy(RIGHT, FAR, 1, left, 6).start()
    y_copy(RIGHT, SRIGHT, 1, sib, 4).start()
    for i in range(half):
        again(sib, i).wait()
    second(pieces_of(SIB, 0, home), pieces_of(LEFT, 0, mid_slot(0)) + pieces_of(RIGHT, 1, mid_slot(1)), first_turned=True)
    y_wait(LEFT, 1)
    y_copy(LEFT, SLEFT, 1, sib, 3).start()
    y_wait(RIGHT, 0)
    y_copy(RIGHT, SRIGHT, 0, sib, 4).start()
    for i in range(half, pieces - EXTRA):
        again(sib, i).wait()
    second(pieces_of(SIB, 1, home)[:-EXTRA], pieces_of(LEFT, 1, mid_slot(0)) + pieces_of(RIGHT, 0, mid_slot(1)))
    for h in range(2):
        y_wait(FAR, h)
        y_copy(FAR, SFAR, h, sib, 7).start()
    for h in range(2):
        y_wait(SLEFT, h)
        y_wait(SRIGHT, 1 - h)
    far_work = pieces_of(FAR, 0, far_slot(0)) + pieces_of(FAR, 1, far_slot(0))
    sfar_work = pieces_of(SFAR, 0, far_slot(1)) + pieces_of(SFAR, 1, far_slot(1))
    second([], pieces_of(SLEFT, 0, mid_slot(2)) + pieces_of(SRIGHT, 1, mid_slot(3)))
    second(far_work[-2:], pieces_of(SLEFT, 1, mid_slot(2)) + pieces_of(SRIGHT, 0, mid_slot(3)) + far_work[:-2])
    for h in range(2):
        y_wait(SFAR, h)
    second(sfar_work[-2:], sfar_work[:-2])
    for j in range(pieces):
        out_buf[j] = jnp.maximum(h2t[j, 0:classes] + acc[part(j), 0:LANES].T[0:classes], 0.0)

    out_copies = [pltpu.make_async_copy(out_buf.at[j], out_hbm.at[:, part(j)], out_sem.at[j]) for j in range(pieces)]
    for copy in out_copies:
        copy.start()
    for group in (0, 1, 2, 3, 4, 7):
        for h in range(2):
            y_copy(OWN, OWN, h, sib, group).wait_send()
    y_copy(OWN, OWN, 0, sib, 5).wait_send()
    y_copy(OWN, OWN, 1, sib, 6).wait_send()
    for copy in out_copies:
        copy.wait()


def solution(mesh):
    n = mesh.shape["row"]
    row_spec = P(("dp", "row"), None)
    full_spec = P(None, None)

    def per_device(adjacency, features, w_first, w_second):
        rows, feat, hidden, classes = features.shape[0], features.shape[1], w_first.shape[1], w_second.shape[1]
        pieces = rows // TILE
        padded = -(-classes // 16) * 16
        resident = adjacency.shape[1] // TILE - 2 * pieces
        flops = 2 * rows * adjacency.shape[1] * (hidden + classes)
        out = pl.pallas_call(
            functools.partial(kernel, n),
            name="gcn",
            out_shape=jax.ShapeDtypeStruct((classes, rows), F32),
            in_specs=[pl.BlockSpec(memory_space=pl.ANY)] * 4,
            out_specs=pl.BlockSpec(memory_space=pl.ANY),
            scratch_shapes=[
                pltpu.VMEM((resident + EXTRA + BLOCKS, rows, TILE), BF16),
                pltpu.VMEM((rows, hidden), F32),
                pltpu.VMEM((H0_RING, feat, TILE), BF16),
                pltpu.VMEM((feat, hidden), BF16),
                pltpu.VMEM((classes, hidden), BF16),
                pltpu.VMEM((padded, hidden), BF16),
                pltpu.VMEM((BLOCKS, 2, pieces // 2, padded, TILE), BF16),
                pltpu.VMEM((pieces, padded, TILE), F32),
                pltpu.VMEM((pieces, classes, TILE), F32),
                pltpu.SemaphoreType.DMA((resident + EXTRA,)),
                pltpu.SemaphoreType.DMA((H0_RING,)),
                pltpu.SemaphoreType.DMA((2,)),
                pltpu.SemaphoreType.DMA((BLOCKS, pieces)),
                pltpu.SemaphoreType.DMA((BLOCKS,)),
                pltpu.SemaphoreType.DMA((BLOCKS, 2)),
                pltpu.SemaphoreType.DMA((BLOCKS, 2)),
                pltpu.SemaphoreType.DMA((pieces,)),
            ],
            compiler_params=pltpu.CompilerParams(
                collective_id=0, has_side_effects=True, vmem_limit_bytes=67_043_328),
            cost_estimate=pl.CostEstimate(
                flops=flops, bytes_accessed=2 * adjacency.size, transcendentals=0),
        )(adjacency, features.T, w_first, w_second.T)
        return out.T

    return jax.shard_map(
        per_device, mesh=mesh, in_specs=(row_spec, row_spec, full_spec, full_spec), out_specs=row_spec,
        check_vma=False)
```
